256 devices in a mesh: seq: 16 (over z, core), head: 16 (over x, y).
Axes of the slice: x: 4, y: 4, z: 8, core: 2. Of those that a mesh axis runs over, the one named last changes fastest.
Arguments:
- queries: bfloat16 [8192, 4096], P('seq', 'head'), may hold values from -6 to 6
- keys: bfloat16 [8192, 1024], P(('seq', 'head')), may hold values from -6 to 6
- values: bfloat16 [8192, 1024], P(('seq', 'head')), may hold values from -3 to 3
- attn_out: bfloat16 [8192, 4096], P('seq', 'head'), may hold values from -1.796875 to 1.796875
- out_grad: bfloat16 [8192, 4096], P('seq', 'head'), may hold values from -6 to 6
- log_norm: float32 [32, 8192], P('head', 'seq'), may hold values from 3.5 to 5.5
- block_layout: int32 [32, 64, 64], P('head'), may hold values 0 or 1
- document_ids: int32 [8192], replicated, may hold values from 0 to 7, never falling along the last dimension, each value on 1 to 4096 neighbouring positions
- block_order: int32 [64], replicated, may hold values from 0 to 63, each once
Outputs:
- query_grad: float32 [8192, 4096], P('seq', 'head')
- key_grad: float32 [8192, 1024], P(('seq', 'head'))
- value_grad: float32 [8192, 1024], P(('seq', 'head'))
The draws below stay inside these ranges and needn't reach their ends.
Inputs may be any that keep to these rules, and one draw needn't show every extreme that they name: `document_ids`: never falls along the sequence position; each document covers 1 to 4096 positions, one exactly 4096. `block_order`: each sequence block once.
All inputs are finite; a program needn't handle non-finite values.
Results may differ from the reference program's by a relative error of at most 0.0029.
Values may be sent and summed in bfloat16 or wider, within the bound.
A program may use at most 128 MiB of HBM per device.

```python
import math
import jax
import jax.numpy as jnp
import numpy as np
from jax import lax

D_HEAD = 128
GROUP = 4
BLOCK = 128
DOCS = 8
HEADS = 32
KV_HEADS = 8
SEQ = 8192
NBLK = 64


def touch_ends(entries, stream_key, low, largest):
    longest = entries.shape.index(max(entries.shape))
    spots = []
    for shift in (0, 1):
        where = [jax.random.randint(jax.random.fold_in(stream_key, axis), (), 0, length) for axis, length in enumerate(entries.shape)]
        where[longest] = (where[longest] + shift) % entries.shape[longest]
        spots.append(tuple(where))
    return entries.at[spots[0]].set(low).at[spots[1]].set(largest)


def steps_of(key, dims, shards, smallest, high):
    def one(axis_at, parts):
        heights = jax.random.uniform(jax.random.fold_in(jax.random.fold_in(key, 6), axis_at), (parts,), jnp.float32, smallest / len(shards), high / len(shards))
        return jnp.repeat(jnp.exp(heights), dims[axis_at] // parts).reshape((-1,) + (1,) * (len(dims) - axis_at - 1))

    loudness = one(*shards[0])
    for cut in shards[1:]:
        loudness = loudness * one(*cut)
    return loudness


def split_up(count, total, most, lean):
    loads = [(1 << 20) // math.isqrt(grade ** lean) + 1 for grade in range(2, count + 1)]
    surplus, counts = total - most - (count - 1), [1] * (count - 1)
    while surplus > 0:
        movable = [i for i in range(count - 1) if counts[i] < most]
        mass, budget = sum([loads[i] for i in movable]), surplus
        for i in movable:
            addition = min(most - counts[i], max(1, budget * loads[i] // mass), surplus)
            counts[i] = counts[i] + addition
            surplus = surplus - addition
    return np.array([most] + counts)


def uneven_parts(own_key, number_of, total, most, skew):
    if number_of == 2:
        one = jax.random.randint(own_key, (), max(1, total - most), min(most, total - 1) + 1)
        return jnp.stack([one, total - one])
    tallies = jnp.asarray(split_up(number_of, total, most, skew), jnp.int32)
    pairs = (number_of - 1) // 2
    source_of, taker = tallies[1:1 + 2 * pairs:2], tallies[2:2 + 2 * pairs:2]
    margin = jnp.minimum(source_of - 1, most - taker)
    shifted = jax.random.randint(jax.random.fold_in(own_key, 1), (pairs,), 0, 1 << 20) % (margin + 1)
    tallies = tallies.at[1:1 + 2 * pairs:2].set(source_of - shifted).at[2:2 + 2 * pairs:2].set(taker + shifted)
    return tallies[jax.random.permutation(jax.random.fold_in(own_key, 2), number_of)]


def bell_draw(key, shape, spread, reach, split=(), kind=jnp.bfloat16):
    drawn = spread * jax.random.normal(key, shape, jnp.float32)
    if split:
        drawn = drawn * steps_of(key, shape, split, -0.22, 0.18)
    return jnp.clip(drawn, -reach, reach).astype(kind)


def setup_inputs(seed: int = 0) -> dict:
    arg_keys = jax.random.split(jax.random.key(seed), 10)
    return {
        "queries": bell_draw(arg_keys[0], (SEQ, HEADS * D_HEAD), 1.0, 6.0, ((0, 16), (1, 16))),
        "keys": bell_draw(arg_keys[1], (SEQ, KV_HEADS * D_HEAD), 1.0, 6.0, ((0, 256),)),
        "values": bell_draw(arg_keys[2], (SEQ, KV_HEADS * D_HEAD), 0.5, 3.0, ((0, 256),)),
        "attn_out": bell_draw(arg_keys[3], (SEQ, HEADS * D_HEAD), 0.3, 1.796875, ((0, 16), (1, 16))),
        "out_grad": bell_draw(arg_keys[4], (SEQ, HEADS * D_HEAD), 1.0, 6.0, ((0, 16), (1, 16))),
        "log_norm": jnp.clip(3.5 + 2.0 * jax.random.uniform(arg_keys[5], (HEADS, SEQ), jnp.float32) ** steps_of(arg_keys[5], (HEADS, SEQ), ((0, 16), (1, 16)), -0.2, 0.2), 3.5, 5.5),
        "block_layout": touch_ends((jax.random.randint(arg_keys[6], (HEADS, NBLK, NBLK), 0, 4) < 3).astype(jnp.int32), jax.random.fold_in(arg_keys[6], 1), 0, 1),
        "document_ids": jnp.searchsorted(jnp.cumsum(uneven_parts(arg_keys[7], DOCS, SEQ, SEQ // 2, 2)), jnp.arange(SEQ), side="right").astype(jnp.int32),
        "block_order": jax.random.permutation(arg_keys[8], NBLK).astype(jnp.int32),
    }


def stored_positions(block_order, document_ids):
    stored = jnp.arange(SEQ, dtype=jnp.int32)
    position = block_order[stored // BLOCK].astype(jnp.int32) * BLOCK + stored % BLOCK
    return position, document_ids[position]


def reference(queries, keys, values, attn_out, out_grad, log_norm, block_layout, document_ids, block_order):
    position, docs = stored_positions(block_order, document_ids)
    blocks = position // BLOCK
    scaling = D_HEAD ** -0.5
    allowed = (position[None, :] <= position[:, None]) & (docs[:, None] == docs[None, :])
    query_heads = queries.reshape(SEQ, HEADS, D_HEAD).transpose(1, 0, 2)
    grad_heads = out_grad.reshape(SEQ, HEADS, D_HEAD).transpose(1, 0, 2)
    out_heads = attn_out.reshape(SEQ, HEADS, D_HEAD).transpose(1, 0, 2)
    key_heads = keys.reshape(SEQ, KV_HEADS, D_HEAD).transpose(1, 0, 2)
    value_heads = values.reshape(SEQ, KV_HEADS, D_HEAD).transpose(1, 0, 2)

    def one_head(head_index):
        query_one = query_heads[head_index]
        grad_one = grad_heads[head_index]
        out_one = out_heads[head_index]
        key_one = key_heads[head_index // GROUP]
        value_one = value_heads[head_index // GROUP]
        layout_one = block_layout[head_index][blocks[:, None], blocks[None, :]] == 1
        visible = allowed & layout_one
        scores = jnp.dot(query_one, key_one.T, preferred_element_type=jnp.float32) * scaling
        weights = jnp.where(visible, jnp.exp(scores - log_norm[head_index][:, None]), 0.0)
        weights_low = weights.astype(jnp.bfloat16)
        value_part = jnp.dot(weights_low.T, grad_one, preferred_element_type=jnp.float32)
        grad_scores = jnp.dot(grad_one, value_one.T, preferred_element_type=jnp.float32)
        delta = jnp.sum(grad_one.astype(jnp.float32) * out_one.astype(jnp.float32), axis=1)
        score_grad = (weights * (grad_scores - delta[:, None])).astype(jnp.bfloat16)
        query_part = jnp.dot(score_grad, key_one, preferred_element_type=jnp.float32)
        key_part = jnp.dot(score_grad.T, query_one, preferred_element_type=jnp.float32)
        return query_part, key_part, value_part

    query_all, key_all, value_all = lax.map(one_head, jnp.arange(HEADS, dtype=jnp.int32))
    query_grad = (query_all * scaling).transpose(1, 0, 2).reshape(SEQ, HEADS * D_HEAD)
    key_sum = key_all.reshape(KV_HEADS, GROUP, SEQ, D_HEAD).sum(axis=1) * scaling
    value_sum = value_all.reshape(KV_HEADS, GROUP, SEQ, D_HEAD).sum(axis=1)
    key_grad = key_sum.transpose(1, 0, 2).reshape(SEQ, KV_HEADS * D_HEAD)
    value_grad = value_sum.transpose(1, 0, 2).reshape(SEQ, KV_HEADS * D_HEAD)
    return (query_grad, key_grad, value_grad)
```

```python
import functools

import jax
import jax.numpy as jnp
from jax import lax
from jax.experimental import pallas as pl
from jax.experimental.pallas import tpu as pltpu
from jax.sharding import PartitionSpec as P

MESH = pl.DeviceIdType.MESH
D = 128
GROUP = 4
BLOCK = 128
NBLK = 64
NZ = 8
TILE = 32
CHUNK_TILES = 4
CHUNK = TILE * CHUNK_TILES
KEYS = NBLK * TILE
PLANE_KEYS = KEYS // NZ
ROWS = 512
NEVER = 1e30
SCALE = D ** (-0.5)
BF16 = jnp.bfloat16
F32 = jnp.float32


def place():
    s = lax.axis_index("seq")
    h = lax.axis_index("head")
    return s, h, s // 2, s % 2, h // 4, h % 4


def send(src, dst, send_sem, recv_sem, seq, head):
    return pltpu.make_async_remote_copy(
        src_ref=src,
        dst_ref=dst,
        send_sem=send_sem,
        recv_sem=recv_sem,
        device_id=(seq, head),
        device_id_type=MESH,
    )


def greet(sources, count):
    barrier = pltpu.get_barrier_semaphore()
    for seq, head, other in sources:
        if other is None:
            pl.semaphore_signal(barrier, inc=1, device_id=(seq, head), device_id_type=MESH)
        else:

            @pl.when(other)
            def _():
                pl.semaphore_signal(barrier, inc=1, device_id=(seq, head), device_id_type=MESH)

    pl.semaphore_wait(barrier, count)


SUBS = ((0, 0), (0, 1), (1, 0), (1, 1))
HALF = PLANE_KEYS // 2


def gather_kernel(
    keys, values, queries, grads, outs, norms, layout,
    kv_all, q_all, g_all, s_all, l_all,
    stats, a_send, a_recv, z_send, z_recv, y_send, y_recv, d_send, d_recv, f_send, f_recv,
):
    s, h, z, c, x, y = place()
    pair = h + 1 - 2 * (y % 2)
    twin = s + 1 - 2 * c
    up = ((z + 1) % NZ) * 2 + c
    down = ((z + NZ - 1) % NZ) * 2 + c
    hp = y % 2
    quarter = hp * 2 + c

    takers = []
    for xg in range(4):
        for yp in range(2):
            seq, head = z * 2 + y % 2, xg * 4 + yp * 2 + y // 2
            takers.append((seq, head, (seq != s) | (head != h)))
    givers = []
    for cg in range(2):
        for xg in range(4):
            seq, head = z * 2 + cg, xg * 4 + quarter
            givers.append((seq, head, (seq != s) | (head != h)))
    own = ((y % 2 == c) & (y // 2 == hp)).astype(jnp.int32)
    greet(
        [(s, pair, None), (twin, h, None), (up, h, None), (down, h, None)] + givers,
        4 + 8 - own,
    )

    slot = c * 4 + x
    a_copies = []
    for g, (seq, head, other) in enumerate(takers):
        for t, src in enumerate((keys, values)):
            copy = send(
                src.at[:, pl.ds(g * D, D)],
                kv_all.at[t, z, pl.ds(pl.multiple_of(slot * TILE, TILE), TILE), :],
                a_send.at[t, g],
                a_recv.at[t, slot],
                seq,
                head,
            )
            pl.when(other)(copy.start)
            a_copies.append((copy, other))

            @pl.when(jnp.logical_not(other))
            def _():
                kv_all[t, z, pl.ds(pl.multiple_of(slot * TILE, TILE), TILE), :] = src[:, g * D : (g + 1) * D]

    y_copies = [
        send(queries, q_all.at[c, hp], y_send.at[0], y_recv.at[0], s, pair),
        send(grads, g_all.at[c, hp], y_send.at[1], y_recv.at[1], s, pair),
        send(layout, l_all.at[hp], y_send.at[2], y_recv.at[2], s, pair),
        send(stats, s_all.at[c, hp], y_send.at[3], y_recv.at[3], s, pair),
    ]
    d_copies = [
        send(queries, q_all.at[c, hp], d_send.at[0], d_recv.at[0], twin, h),
        send(grads, g_all.at[c, hp], d_send.at[1], d_recv.at[1], twin, h),
        send(stats, s_all.at[c, hp], d_send.at[2], d_recv.at[2], twin, h),
    ]
    for copy in y_copies[:2] + d_copies[:2]:
        copy.start()

    ones = jnp.ones((8, D), BF16)
    for hh in range(2):
        stats[hh * 4 : hh * 4 + 4, :] = norms[hh * 4 : hh * 4 + 4, :]
        for rb in range(4):
            at = (slice(rb * BLOCK, (rb + 1) * BLOCK), slice(hh * D, (hh + 1) * D))
            product = grads[at].astype(F32) * outs[at].astype(F32)
            high = product.astype(BF16)
            low = (product - high.astype(F32)).astype(BF16)
            dims = (((1,), (1,)), ((), ()))
            total = lax.dot_general(ones, high, dims, preferred_element_type=F32)
            total = total + lax.dot_general(ones, low, dims, preferred_element_type=F32)
            stats[8 + hh * 4 + rb : 9 + hh * 4 + rb, :] = total[0:1, :]
    for copy in (y_copies[2], y_copies[3], d_copies[2]):
        copy.start()
    s_all[c, hp] = stats[...]
    l_all[hp] = layout[...]
    q_all[c, hp] = queries[...]
    g_all[c, hp] = grads[...]

    def piece(t, half, plane):
        return kv_all.at[t, plane, pl.ds(half * HALF, HALF), :]

    def hop(way, step, sub):
        t, half = SUBS[sub]
        origin = (z + NZ - (step - 1)) % NZ if way == 0 else (z + step - 1) % NZ
        return send(
            piece(t, half, origin), piece(t, half, origin),
            z_send.at[way, step - 1, sub], z_recv.at[way, step - 1, sub],
            up if way == 0 else down, h,
        )

    def carries(way, step, sub):
        return step < 4 or (step == 4 and SUBS[sub][0] == way)

    z_copies = {}
    for sub, (t, half) in enumerate(SUBS):
        for k in range(4):
            at = half * 4 + k
            seq, head, other = givers[at]
            landed = send(
                keys.at[:, pl.ds(0, D)], kv_all.at[t, z, pl.ds(at * TILE, TILE), :],
                a_send.at[t, 0], a_recv.at[t, at], seq, head,
            )
            pl.when(other)(landed.wait_recv)
        for way in range(2):
            z_copies[way, 1, sub] = hop(way, 1, sub)
            z_copies[way, 1, sub].start()

    forwards = []

    def pass_on(k, ref_all):
        y_copies[k].wait_recv()
        copy = send(ref_all.at[c, 1 - hp], ref_all.at[c, 1 - hp], f_send.at[len(forwards)], f_recv.at[len(forwards)], twin, h)
        copy.start()
        forwards.append(copy)

    for step in range(1, 5):
        for sub in range(4):
            for way in range(2):
                if not carries(way, step, sub):
                    continue
                z_copies[way, step, sub].wait_recv()
                if carries(way, step + 1, sub):
                    z_copies[way, step + 1, sub] = hop(way, step + 1, sub)
                    z_copies[way, step + 1, sub].start()
        if step == 1:
            pass_on(0, q_all)
        if step == 3:
            pass_on(1, g_all)
            pass_on(3, s_all)
            y_copies[2].wait_recv()

    for copy in d_copies + forwards:
        copy.wait_recv()
    for copy, other in a_copies:
        pl.when(other)(copy.wait_send)
    for copy in list(z_copies.values()) + y_copies + d_copies + forwards:
        copy.wait_send()


def gather(keys, values, queries, grads, outs, norms, layout):
    vmem = pl.BlockSpec(memory_space=pltpu.VMEM)
    dma = pltpu.SemaphoreType.DMA
    return pl.pallas_call(
        gather_kernel,
        name="exchange_in",
        out_shape=(
            jax.ShapeDtypeStruct((2, NZ, PLANE_KEYS, D), BF16),
            jax.ShapeDtypeStruct((2, 2, ROWS, 2 * D), BF16),
            jax.ShapeDtypeStruct((2, 2, ROWS, 2 * D), BF16),
            jax.ShapeDtypeStruct((2, 2, 16, BLOCK), F32),
            jax.ShapeDtypeStruct((2, 2 * NBLK, NBLK), BF16),
        ),
        in_specs=[vmem] * 7,
        out_specs=(vmem,) * 5,
        scratch_shapes=[
            pltpu.VMEM((16, BLOCK), F32),
            dma((2, 8)), dma((2, 8)),
            dma((2, 4, 4)), dma((2, 4, 4)),
            dma((4,)), dma((4,)),
            dma((3,)), dma((3,)),
            dma((3,)), dma((3,)),
        ],
        compiler_params=pltpu.CompilerParams(collective_id=0, has_side_effects=True),
    )(keys, values, queries, grads, outs, norms, layout)


def attend_kernel(
    where_ref, order, first, kv, q_all, g_all, s_all, l_all, start,
    dq, dkv,
    ks, vs, dks, dvs, lay, pick, bias, qs, gs, dqt,
):
    z, quarter = where_ref[0], where_ref[1]

    def sort(sb, _):
        to = pl.ds(pl.multiple_of(order[sb] * TILE, TILE), TILE)
        at = pl.ds(pl.multiple_of(sb * TILE, TILE), TILE)
        ks[to, :] = kv[0, at, :]
        vs[to, :] = kv[1, at, :]
        return 0

    lax.fori_loop(0, NBLK, sort, 0, unroll=8)
    dks[...] = jnp.zeros_like(dks)
    dvs[...] = jnp.zeros_like(dvs)
    for hp in range(2):
        lay[hp * 2 * NBLK : (hp + 1) * 2 * NBLK, :] = l_all[hp].astype(F32)
    pick[...] = jnp.zeros_like(pick)
    spread = (
        lax.broadcasted_iota(jnp.int32, (8, GROUP * BLOCK), 1) // BLOCK
        == lax.broadcasted_iota(jnp.int32, (8, GROUP * BLOCK), 0)
    ).astype(F32)
    nt = (((1,), (1,)), ((), ()))
    tn = (((0,), (0,)), ((), ()))
    row = lax.broadcasted_iota(jnp.int32, (TILE, GROUP * BLOCK), 0)

    def one_block(i, _):
        cb, rb = i // 4, i % 4
        block = order[z * 8 + i]
        rows = pl.ds(pl.multiple_of(rb * BLOCK, BLOCK), BLOCK)
        norm, delta = [], []
        for head in range(GROUP):
            hp, hh = head // 2, head % 2
            qs[head * BLOCK : (head + 1) * BLOCK, :] = q_all[cb, hp, rows, hh * D : (hh + 1) * D]
            gs[head * BLOCK : (head + 1) * BLOCK, :] = g_all[cb, hp, rows, hh * D : (hh + 1) * D]
            norm.append(s_all[cb, hp, pl.ds(hh * 4 + rb, 1), :])
            delta.append(s_all[cb, hp, pl.ds(8 + hh * 4 + rb, 1), :])
            pick[head : head + 1, :] = lay[pl.ds(head * NBLK + block, 1), :]
        norm = jnp.concatenate(norm, axis=1)
        delta = jnp.concatenate(delta, axis=1)
        seen = lax.dot_general(pick[...], spread, tn, preferred_element_type=F32)
        bias[...] = jnp.where(seen > 0.5, norm, NEVER)
        begin = start[pl.ds(block, 1), :]
        begin = jnp.concatenate([begin] * GROUP, axis=1)
        last = block * BLOCK + lax.broadcasted_iota(jnp.int32, (1, GROUP * BLOCK), 1) % BLOCK
        dqt[...] = jnp.zeros_like(dqt)

        def one_chunk(ch, _):
            at = pl.ds(pl.multiple_of(ch * CHUNK, CHUNK), CHUNK)
            kc, vc = ks[at, :], vs[at, :]
            scores = lax.dot_general(kc, qs[...], nt, preferred_element_type=F32)
            grad_scores = lax.dot_general(vc, gs[...], nt, preferred_element_type=F32)
            low, score_grad = [], []
            for t in range(CHUNK_TILES):
                part = slice(t * TILE, (t + 1) * TILE)
                tile = ch * CHUNK_TILES + t
                position = row + (tile * BLOCK + quarter * TILE)
                visible = (position >= begin) & (position <= last)
                weights = jnp.exp(scores[part, :] * SCALE - bias[pl.ds(tile, 1), :])
                weights = jnp.where(visible, weights, 0.0)
                low.append(weights.astype(BF16))
                score_grad.append((weights * (grad_scores[part, :] - delta)).astype(BF16))
            low = jnp.concatenate(low, axis=0)
            score_grad = jnp.concatenate(score_grad, axis=0)
            dvs[at, :] += jnp.dot(low, gs[...], preferred_element_type=F32)
            dks[at, :] += jnp.dot(score_grad, qs[...], preferred_element_type=F32)
            dqt[...] += lax.dot_general(kc, score_grad, tn, preferred_element_type=F32)
            return 0

        lax.fori_loop(first[block] // CHUNK_TILES, block // CHUNK_TILES + 1, one_chunk, 0)
        for head in range(GROUP):
            hp, hh = head // 2, head % 2
            block_grad = dqt[:, head * BLOCK : (head + 1) * BLOCK].T
            dq[cb, hp, rows, hh * D : (hh + 1) * D] = block_grad * SCALE
        return 0

    lax.fori_loop(0, 8, one_block, 0)

    def unsort(sb, _):
        at = pl.ds(pl.multiple_of(order[sb] * TILE, TILE), TILE)
        to = pl.ds(pl.multiple_of(sb * TILE, TILE), TILE)
        dkv[0, to, :] = dks[at, :]
        dkv[1, to, :] = dvs[at, :]
        return 0

    lax.fori_loop(0, NBLK, unsort, 0, unroll=8)


def attend(where, order, first, kv, q_all, g_all, s_all, l_all, start):
    vmem = pl.BlockSpec(memory_space=pltpu.VMEM)
    smem = pl.BlockSpec(memory_space=pltpu.SMEM)
    return pl.pallas_call(
        attend_kernel,
        name="attend",
        out_shape=(
            jax.ShapeDtypeStruct((2, 2, ROWS, 2 * D), F32),
            jax.ShapeDtypeStruct((2, KEYS, D), F32),
        ),
        in_specs=[smem] * 3 + [vmem] * 6,
        out_specs=(vmem, vmem),
        scratch_shapes=[
            pltpu.VMEM((KEYS, D), BF16),
            pltpu.VMEM((KEYS, D), BF16),
            pltpu.VMEM((KEYS, D), F32),
            pltpu.VMEM((KEYS, D), F32),
            pltpu.VMEM((GROUP * NBLK, NBLK), F32),
            pltpu.VMEM((8, NBLK), F32),
            pltpu.VMEM((NBLK, GROUP * BLOCK), F32),
            pltpu.VMEM((GROUP * BLOCK, D), BF16),
            pltpu.VMEM((GROUP * BLOCK, D), BF16),
            pltpu.VMEM((D, GROUP * BLOCK), F32),
        ],
    )(where, order, first, kv, q_all, g_all, s_all, l_all, start)


def scatter_kernel(
    dq_part, dkv,
    dq, dk, dv,
    twin_in, pair_out, pair_in, z_out, z_in, fin, own_in,
    d_send, d_recv, y_send, y_recv, z_send, z_recv, a_send, a_recv,
):
    s, h, z, c, x, y = place()
    pair = h + 1 - 2 * (y % 2)
    twin = s + 1 - 2 * c
    up = ((z + 1) % NZ) * 2 + c
    down = ((z + NZ - 1) % NZ) * 2 + c
    hp = y % 2
    quarter = hp * 2 + c

    owners = []
    for cg in range(2):
        for xg in range(4):
            seq, head = z * 2 + cg, xg * 4 + quarter
            owners.append((seq, head, (seq != s) | (head != h)))
    makers = []
    for xg in range(4):
        for yp in range(2):
            seq, head = z * 2 + y % 2, xg * 4 + yp * 2 + y // 2
            makers.append((seq, head, (seq != s) | (head != h)))
    own = ((y % 2 == c) & (y // 2 == hp)).astype(jnp.int32)
    greet(
        [(s, pair, None), (twin, h, None), (up, h, None), (down, h, None)] + makers,
        4 + 8 - own,
    )

    d_copy = send(dq_part.at[1 - c], twin_in, d_send.at[0], d_recv.at[0], twin, h)
    d_copy.start()

    def rows_of(plane, half):
        return pl.ds(pl.multiple_of(plane * PLANE_KEYS + half * HALF, HALF), HALF)

    z_copies = {}

    def hop(way, step, sub):
        t, half = SUBS[sub]
        target = (z + 5 - step) % NZ if way == 0 else (z + NZ - (5 - step)) % NZ
        value = dkv[t, rows_of(target, half), :]
        if (way, step - 1, sub) in z_copies:
            z_copies[way, step - 1, sub].wait_recv()
            value = value + z_in[way, step - 2, sub].astype(F32)
        z_out[way, step - 1, sub] = value.astype(BF16)
        copy = send(
            z_out.at[way, step - 1, sub], z_in.at[way, step - 1, sub],
            z_send.at[way, step - 1, sub], z_recv.at[way, step - 1, sub],
            up if way == 0 else down, h,
        )
        copy.start()
        z_copies[way, step, sub] = copy

    for sub, (t, half) in enumerate(SUBS):
        hop(t, 1, sub)
    for sub, (t, half) in enumerate(SUBS):
        hop(1 - t, 2, sub)

    d_copy.wait_recv()
    pair_out[...] = (dq_part[c, 1 - hp] + twin_in[1 - hp]).astype(BF16)
    y_copy = send(pair_out, pair_in, y_send.at[0], y_recv.at[0], s, pair)
    y_copy.start()

    for sub, (t, half) in enumerate(SUBS):
        hop(t, 2, sub)
    dq[...] = dq_part[c, hp] + twin_in[hp]
    for step in (3, 4):
        for sub in range(4):
            for way in range(2):
                hop(way, step, sub)

    a_copies = []
    for half in range(2):
        for t in range(2):
            sub = t * 2 + half
            value = dkv[t, rows_of(z, half), :]
            for way in range(2):
                z_copies[way, 4, sub].wait_recv()
                value = value + z_in[way, 3, sub].astype(F32)
            if t == 0:
                value = value * SCALE
            for k in range(4):
                fin[half * 4 + k, t] = value[k * TILE : (k + 1) * TILE, :]
        for k in range(4):
            seq, head, other = owners[half * 4 + k]
            g = x * 2 + y // 2
            copy = send(
                fin.at[half * 4 + k], own_in.at[g],
                a_send.at[half * 4 + k], a_recv.at[g], seq, head,
            )
            pl.when(other)(copy.start)
            a_copies.append((copy, other))

            @pl.when(jnp.logical_not(other))
            def _():
                own_in[g] = fin[half * 4 + k]

    y_copy.wait_recv()
    dq[...] += pair_in[...].astype(F32)

    for g, (seq, head, other) in enumerate(makers):
        landed = send(fin.at[0], own_in.at[g], a_send.at[0], a_recv.at[g], seq, head)
        pl.when(other)(landed.wait_recv)
        dk[:, g * D : (g + 1) * D] = own_in[g, 0]
        dv[:, g * D : (g + 1) * D] = own_in[g, 1]

    for copy, other in a_copies:
        pl.when(other)(copy.wait_send)
    for copy in list(z_copies.values()) + [d_copy, y_copy]:
        copy.wait_send()


def scatter(dq_part, dkv):
    vmem = pl.BlockSpec(memory_space=pltpu.VMEM)
    dma = pltpu.SemaphoreType.DMA
    return pl.pallas_call(
        scatter_kernel,
        name="exchange_out",
        out_shape=(
            jax.ShapeDtypeStruct((ROWS, 2 * D), F32),
            jax.ShapeDtypeStruct((TILE, 8 * D), F32),
            jax.ShapeDtypeStruct((TILE, 8 * D), F32),
        ),
        in_specs=[vmem] * 2,
        out_specs=(vmem,) * 3,
        scratch_shapes=[
            pltpu.VMEM((2, ROWS, 2 * D), F32),
            pltpu.VMEM((ROWS, 2 * D), BF16),
            pltpu.VMEM((ROWS, 2 * D), BF16),
            pltpu.VMEM((2, 4, 4, HALF, D), BF16),
            pltpu.VMEM((2, 4, 4, HALF, D), BF16),
            pltpu.VMEM((8, 2, TILE, D), F32),
            pltpu.VMEM((8, 2, TILE, D), F32),
            dma((1,)), dma((1,)),
            dma((1,)), dma((1,)),
            dma((2, 4, 4)), dma((2, 4, 4)),
            dma((8,)), dma((8,)),
        ],
        compiler_params=pltpu.CompilerParams(collective_id=1, has_side_effects=True),
    )(dq_part, dkv)


def body(
    queries, keys, values, attn_out, out_grad, log_norm, block_layout, document_ids, block_order
):
    _, _, z, c, _, y = place()
    where = jnp.stack([z, (y % 2) * 2 + c]).astype(jnp.int32)
    below = jnp.sum(
        (document_ids[None, :] < jnp.arange(8, dtype=jnp.int32)[:, None]).astype(jnp.int32), axis=1
    )
    ids = document_ids.reshape(NBLK, BLOCK)
    start = jnp.zeros_like(ids)
    for d in range(1, 8):
        start = jnp.where(ids == d, below[d], start)
    first = start[:, 0] // BLOCK
    kv, q_all, g_all, s_all, l_all = gather(
        keys,
        values,
        queries,
        out_grad,
        attn_out,
        log_norm.reshape(8, BLOCK),
        block_layout.reshape(2 * NBLK, NBLK).astype(BF16),
    )
    dq_part, dkv = attend(
        where, block_order, first, kv.reshape(2, KEYS, D), q_all, g_all, s_all, l_all, start
    )
    return scatter(dq_part, dkv)


def solution(mesh):
    in_specs = (
        P("seq", "head"),
        P(("seq", "head"), None),
        P(("seq", "head"), None),
        P("seq", "head"),
        P("seq", "head"),
        P("head", "seq"),
        P("head", None, None),
        P(),
        P(),
    )
    out_specs = (P("seq", "head"), P(("seq", "head"), None), P(("seq", "head"), None))
    return jax.shard_map(body, mesh=mesh, in_specs=in_specs, out_specs=out_specs, check_vma=False)
```

```python
import functools

import jax
import jax.numpy as jnp
from jax import lax
from jax.experimental import pallas as pl
from jax.experimental.pallas import tpu as pltpu
from jax.sharding import PartitionSpec as P

MESH = pl.DeviceIdType.MESH
D = 128
GROUP = 4
BLOCK = 128
NBLK = 64
NZ = 8
TILE = 32
CHUNK_TILES = 8
CHUNK = TILE * CHUNK_TILES
KEYS = NBLK * TILE
PADDED = NBLK + CHUNK_TILES
PLANE_KEYS = KEYS // NZ
ROWS = 512
NEVER = 1e30
SCALE = D ** (-0.5)
LOG2E = 1.4426950408889634
MIB = 1 << 20
IN_VMEM = 12 * MIB
ATTEND_VMEM = 24 * MIB
OUT_VMEM = 16 * MIB
BF16 = jnp.bfloat16
F32 = jnp.float32


def place():
    s = lax.axis_index("seq")
    h = lax.axis_index("head")
    return s, h, s // 2, s % 2, h // 4, h % 4


def send(src, dst, send_sem, recv_sem, seq, head):
    return pltpu.make_async_remote_copy(
        src_ref=src,
        dst_ref=dst,
        send_sem=send_sem,
        recv_sem=recv_sem,
        device_id=(seq, head),
        device_id_type=MESH,
    )


def greet(sources, count):
    barrier = pltpu.get_barrier_semaphore()
    for seq, head, other in sources:
        if other is None:
            pl.semaphore_signal(barrier, inc=1, device_id=(seq, head), device_id_type=MESH)
        else:

            @pl.when(other)
            def _():
                pl.semaphore_signal(barrier, inc=1, device_id=(seq, head), device_id_type=MESH)

    pl.semaphore_wait(barrier, count)


SUBS = ((0, 0), (0, 1), (1, 0), (1, 1))
HALF = PLANE_KEYS // 2


def gather_kernel(
    keys, values, queries, grads, outs, norms, layout, ids,
    kv_all, q_all, g_all, s_all, l_all, below,
    stats, lay, a_send, a_recv, z_send, z_recv, y_send, y_recv, d_send, d_recv, f_send, f_recv,
):
    s, h, z, c, x, y = place()
    pair = h + 1 - 2 * (y % 2)
    twin = s + 1 - 2 * c
    up = ((z + 1) % NZ) * 2 + c
    down = ((z + NZ - 1) % NZ) * 2 + c
    hp = y % 2
    quarter = hp * 2 + c

    takers = []
    for xg in range(4):
        for yp in range(2):
            seq, head = z * 2 + y % 2, xg * 4 + yp * 2 + y // 2
            takers.append((seq, head, (seq != s) | (head != h)))
    givers = []
    for cg in range(2):
        for xg in range(4):
            seq, head = z * 2 + cg, xg * 4 + quarter
            givers.append((seq, head, (seq != s) | (head != h)))
    own = ((y % 2 == c) & (y // 2 == hp)).astype(jnp.int32)
    greet(
        [(s, pair, None), (twin, h, None), (up, h, None), (down, h, None)] + givers,
        4 + 8 - own,
    )

    slot = c * 4 + x
    a_copies = []
    for g, (seq, head, other) in enumerate(takers):
        for t, src in enumerate((keys, values)):
            copy = send(
                src.at[:, pl.ds(g * D, D)],
                kv_all.at[t, z, pl.ds(pl.multiple_of(slot * TILE, TILE), TILE), :],
                a_send.at[t, g],
                a_recv.at[t, slot],
                seq,
                head,
            )
            pl.when(other)(copy.start)
            a_copies.append((copy, other))

            @pl.when(jnp.logical_not(other))
            def _():
                kv_all[t, z, pl.ds(pl.multiple_of(slot * TILE, TILE), TILE), :] = src[:, g * D : (g + 1) * D]

    y_copies = [
        send(queries, q_all.at[c, hp], y_send.at[0], y_recv.at[0], s, pair),
        send(grads, g_all.at[c, hp], y_send.at[1], y_recv.at[1], s, pair),
        send(lay, l_all.at[hp], y_send.at[2], y_recv.at[2], s, pair),
        send(stats, s_all.at[c, hp], y_send.at[3], y_recv.at[3], s, pair),
    ]
    d_copies = [
        send(queries, q_all.at[c, hp], d_send.at[0], d_recv.at[0], twin, h),
        send(grads, g_all.at[c, hp], d_send.at[1], d_recv.at[1], twin, h),
        send(stats, s_all.at[c, hp], d_send.at[2], d_recv.at[2], twin, h),
    ]
    for copy in y_copies[:2] + d_copies[:2]:
        copy.start()

    ones = jnp.ones((8, D), BF16)
    for hh in range(2):
        lay[hh * NBLK : (hh + 1) * NBLK, :] = layout[hh].astype(F32).astype(BF16)
        for rb in range(4):
            stats[hh * 4 + rb : hh * 4 + rb + 1, :] = norms[hh : hh + 1, rb * BLOCK : (rb + 1) * BLOCK]
            at = (slice(rb * BLOCK, (rb + 1) * BLOCK), slice(hh * D, (hh + 1) * D))
            product = grads[at].astype(F32) * outs[at].astype(F32)
            high = product.astype(BF16)
            low = (product - high.astype(F32)).astype(BF16)
            dims = (((1,), (1,)), ((), ()))
            total = lax.dot_general(ones, high, dims, preferred_element_type=F32)
            total = total + lax.dot_general(ones, low, dims, preferred_element_type=F32)
            stats[8 + hh * 4 + rb : 9 + hh * 4 + rb, :] = total[0:1, :]
    for copy in (y_copies[2], y_copies[3], d_copies[2]):
        copy.start()
    s_all[c, hp] = stats[...]
    l_all[hp] = lay[...]
    q_all[c, hp] = queries[...]
    g_all[c, hp] = grads[...]
    below[0] = 0
    for d in range(1, 8):
        below[d] = jnp.sum((ids[...] < d).astype(F32)).astype(jnp.int32)

    def piece(t, half, plane):
        return kv_all.at[t, plane, pl.ds(half * HALF, HALF), :]

    def hop(way, step, sub):
        t, half = SUBS[sub]
        origin = (z + NZ - (step - 1)) % NZ if way == 0 else (z + step - 1) % NZ
        return send(
            piece(t, half, origin), piece(t, half, origin),
            z_send.at[way, step - 1, sub], z_recv.at[way, step - 1, sub],
            up if way == 0 else down, h,
        )

    def carries(way, step, sub):
        return step < 4 or (step == 4 and SUBS[sub][0] == way)

    z_copies = {}
    for sub, (t, half) in enumerate(SUBS):
        for k in range(4):
            at = half * 4 + k
            seq, head, other = givers[at]
            landed = send(
                keys.at[:, pl.ds(0, D)], kv_all.at[t, z, pl.ds(at * TILE, TILE), :],
                a_send.at[t, 0], a_recv.at[t, at], seq, head,
            )
            pl.when(other)(landed.wait_recv)
        for way in range(2):
            z_copies[way, 1, sub] = hop(way, 1, sub)
            z_copies[way, 1, sub].start()

    forwards = []

    def pass_on(k, ref_all):
        y_copies[k].wait_recv()
        copy = send(ref_all.at[c, 1 - hp], ref_all.at[c, 1 - hp], f_send.at[len(forwards)], f_recv.at[len(forwards)], twin, h)
        copy.start()
        forwards.append(copy)

    for step in range(1, 5):
        for sub in range(4):
            for way in range(2):
                if not carries(way, step, sub):
                    continue
                z_copies[way, step, sub].wait_recv()
                if carries(way, step + 1, sub):
                    z_copies[way, step + 1, sub] = hop(way, step + 1, sub)
                    z_copies[way, step + 1, sub].start()
        if step == 1:
            pass_on(0, q_all)
        if step == 3:
            pass_on(1, g_all)
            pass_on(3, s_all)
            y_copies[2].wait_recv()

    for copy in d_copies + forwards:
        copy.wait_recv()
    for copy, other in a_copies:
        pl.when(other)(copy.wait_send)
    for copy in list(z_copies.values()) + y_copies + d_copies + forwards:
        copy.wait_send()


def gather(keys, values, queries, grads, outs, norms, layout, ids):
    vmem = pl.BlockSpec(memory_space=pltpu.VMEM)
    dma = pltpu.SemaphoreType.DMA
    return pl.pallas_call(
        gather_kernel,
        name="exchange_in",
        out_shape=(
            jax.ShapeDtypeStruct((2, NZ, PLANE_KEYS, D), BF16),
            jax.ShapeDtypeStruct((2, 2, ROWS, 2 * D), BF16),
            jax.ShapeDtypeStruct((2, 2, ROWS, 2 * D), BF16),
            jax.ShapeDtypeStruct((2, 2, 16, BLOCK), F32),
            jax.ShapeDtypeStruct((2, 2 * NBLK, NBLK), BF16),
            jax.ShapeDtypeStruct((8,), jnp.int32),
        ),
        in_specs=[vmem] * 8,
        out_specs=(vmem,) * 5 + (pl.BlockSpec(memory_space=pltpu.SMEM),),
        scratch_shapes=[
            pltpu.VMEM((16, BLOCK), F32),
            pltpu.VMEM((2 * NBLK, NBLK), BF16),
            dma((2, 8)), dma((2, 8)),
            dma((2, 4, 4)), dma((2, 4, 4)),
            dma((4,)), dma((4,)),
            dma((3,)), dma((3,)),
            dma((3,)), dma((3,)),
        ],
        compiler_params=pltpu.CompilerParams(collective_id=0, has_side_effects=True, vmem_limit_bytes=IN_VMEM),
    )(keys, values, queries, grads, outs, norms, layout, ids)


def attend_kernel(
    order, below, kv, q_all, g_all, s_all, l_all,
    dq, dkv,
    ks, vs, dks, dvs, lay, pick, bias, qs, gs, dqt,
):
    _, _, z, c, _, y = place()
    quarter = (y % 2) * 2 + c
    edge = pl.ds(KEYS, CHUNK)
    ks[edge, :] = jnp.zeros((CHUNK, D), BF16)
    vs[edge, :] = jnp.zeros((CHUNK, D), BF16)
    bias[NBLK:, :] = jnp.full((CHUNK_TILES, GROUP * BLOCK), NEVER, F32)

    def sort(sb, _):
        to = pl.ds(pl.multiple_of(order[sb] * TILE, TILE), TILE)
        at = pl.ds(pl.multiple_of(sb * TILE, TILE), TILE)
        ks[to, :] = kv[0, at, :]
        vs[to, :] = kv[1, at, :]
        return 0

    lax.fori_loop(0, NBLK, sort, 0, unroll=8)
    dks[...] = jnp.zeros_like(dks)
    dvs[...] = jnp.zeros_like(dvs)
    for hp in range(2):
        lay[hp * 2 * NBLK : (hp + 1) * 2 * NBLK, :] = l_all[hp].astype(F32)
    pick[...] = jnp.zeros_like(pick)
    spread = (
        lax.broadcasted_iota(jnp.int32, (8, GROUP * BLOCK), 1) // BLOCK
        == lax.broadcasted_iota(jnp.int32, (8, GROUP * BLOCK), 0)
    ).astype(F32)
    nt = (((1,), (1,)), ((), ()))
    tn = (((0,), (0,)), ((), ()))
    row = lax.broadcasted_iota(jnp.int32, (TILE, GROUP * BLOCK), 0)

    def one_block(i, _):
        cb, rb = i // 4, i % 4
        block = order[z * 8 + i]
        rows = pl.ds(pl.multiple_of(rb * BLOCK, BLOCK), BLOCK)
        norm, delta = [], []
        for head in range(GROUP):
            hp, hh = head // 2, head % 2
            qs[head * BLOCK : (head + 1) * BLOCK, :] = q_all[cb, hp, rows, hh * D : (hh + 1) * D]
            gs[head * BLOCK : (head + 1) * BLOCK, :] = g_all[cb, hp, rows, hh * D : (hh + 1) * D]
            norm.append(s_all[cb, hp, pl.ds(hh * 4 + rb, 1), :])
            delta.append(s_all[cb, hp, pl.ds(8 + hh * 4 + rb, 1), :])
            pick[head : head + 1, :] = lay[pl.ds(head * NBLK + block, 1), :]
        norm = jnp.concatenate(norm, axis=1)
        delta = jnp.concatenate(delta, axis=1)
        seen = lax.dot_general(pick[...], spread, tn, preferred_element_type=F32)
        bias[:NBLK, :] = jnp.where(seen > 0.5, norm * LOG2E, NEVER)
        last = block * BLOCK + lax.broadcasted_iota(jnp.int32, (1, GROUP * BLOCK), 1) % BLOCK
        begin = jnp.zeros_like(last)
        first = 0
        for d in range(1, 8):
            begin = jnp.where(last >= below[d], below[d], begin)
            first = jnp.where(block * BLOCK >= below[d], below[d], first)
        first = first // BLOCK
        dqt[...] = jnp.zeros_like(dqt)

        def one_chunk(ch, _):
            tile0 = first + ch * CHUNK_TILES
            at = pl.ds(pl.multiple_of(tile0 * TILE, TILE), CHUNK)
            kc, vc = ks[at, :], vs[at, :]
            scores = lax.dot_general(kc, qs[...], nt, preferred_element_type=F32)
            grad_scores = lax.dot_general(vc, gs[...], nt, preferred_element_type=F32)
            low, score_grad = [], []
            for t in range(CHUNK_TILES):
                part = slice(t * TILE, (t + 1) * TILE)
                tile = tile0 + t
                position = row + (tile * BLOCK + quarter * TILE)
                visible = (position >= begin) & (position <= last)
                weights = jnp.exp2(scores[part, :] * (SCALE * LOG2E) - bias[pl.ds(tile, 1), :])
                weights = jnp.where(visible, weights, 0.0)
                low.append(weights.astype(BF16))
                score_grad.append((weights * (grad_scores[part, :] - delta)).astype(BF16))
            low = jnp.concatenate(low, axis=0)
            score_grad = jnp.concatenate(score_grad, axis=0)
            dvs[at, :] += jnp.dot(low, gs[...], preferred_element_type=F32)
            dks[at, :] += jnp.dot(score_grad, qs[...], preferred_element_type=F32)
            dqt[...] += lax.dot_general(kc, score_grad, tn, preferred_element_type=F32)
            return 0

        lax.fori_loop(0, (block - first) // CHUNK_TILES + 1, one_chunk, 0)
        for head in range(GROUP):
            hp, hh = head // 2, head % 2
            block_grad = dqt[:, head * BLOCK : (head + 1) * BLOCK].T
            dq[cb, hp, rows, hh * D : (hh + 1) * D] = block_grad * SCALE
        return 0

    lax.fori_loop(0, 8, one_block, 0)

    def unsort(sb, _):
        at = pl.ds(pl.multiple_of(order[sb] * TILE, TILE), TILE)
        to = pl.ds(pl.multiple_of(sb * TILE, TILE), TILE)
        dkv[0, to, :] = dks[at, :]
        dkv[1, to, :] = dvs[at, :]
        return 0

    lax.fori_loop(0, NBLK, unsort, 0, unroll=8)


def attend(order, below, kv, q_all, g_all, s_all, l_all):
    vmem = pl.BlockSpec(memory_space=pltpu.VMEM)
    smem = pl.BlockSpec(memory_space=pltpu.SMEM)
    return pl.pallas_call(
        attend_kernel,
        name="attend",
        out_shape=(
            jax.ShapeDtypeStruct((2, 2, ROWS, 2 * D), F32),
            jax.ShapeDtypeStruct((2, KEYS, D), F32),
        ),
        in_specs=[smem] * 2 + [vmem] * 5,
        out_specs=(vmem, vmem),
        scratch_shapes=[
            pltpu.VMEM((PADDED * TILE, D), BF16),
            pltpu.VMEM((PADDED * TILE, D), BF16),
            pltpu.VMEM((PADDED * TILE, D), F32),
            pltpu.VMEM((PADDED * TILE, D), F32),
            pltpu.VMEM((GROUP * NBLK, NBLK), F32),
            pltpu.VMEM((8, NBLK), F32),
            pltpu.VMEM((PADDED, GROUP * BLOCK), F32),
            pltpu.VMEM((GROUP * BLOCK, D), BF16),
            pltpu.VMEM((GROUP * BLOCK, D), BF16),
            pltpu.VMEM((D, GROUP * BLOCK), F32),
        ],
        compiler_params=pltpu.CompilerParams(vmem_limit_bytes=ATTEND_VMEM),
    )(order, below, kv, q_all, g_all, s_all, l_all)


def scatter_kernel(
    dq_part, dkv,
    dq, pair_in, own_in,
    twin_in, pair_out, z_out, z_in, fin,
    d_send, d_recv, y_send, y_recv, z_send, z_recv, a_send, a_recv,
):
    s, h, z, c, x, y = place()
    pair = h + 1 - 2 * (y % 2)
    twin = s + 1 - 2 * c
    up = ((z + 1) % NZ) * 2 + c
    down = ((z + NZ - 1) % NZ) * 2 + c
    hp = y % 2
    quarter = hp * 2 + c

    owners = []
    for cg in range(2):
        for xg in range(4):
            seq, head = z * 2 + cg, xg * 4 + quarter
            owners.append((seq, head, (seq != s) | (head != h)))
    makers = []
    for xg in range(4):
        for yp in range(2):
            seq, head = z * 2 + y % 2, xg * 4 + yp * 2 + y // 2
            makers.append((seq, head, (seq != s) | (head != h)))
    own = ((y % 2 == c) & (y // 2 == hp)).astype(jnp.int32)
    greet(
        [(s, pair, None), (twin, h, None), (up, h, None), (down, h, None)] + makers,
        4 + 8 - own,
    )

    d_copy = send(dq_part.at[1 - c], twin_in, d_send.at[0], d_recv.at[0], twin, h)
    d_copy.start()

    def rows_of(plane, half):
        return pl.ds(pl.multiple_of(plane * PLANE_KEYS + half * HALF, HALF), HALF)

    z_copies = {}

    def hop(way, step, sub):
        t, half = SUBS[sub]
        target = (z + 5 - step) % NZ if way == 0 else (z + NZ - (5 - step)) % NZ
        value = dkv[t, rows_of(target, half), :]
        if (way, step - 1, sub) in z_copies:
            z_copies[way, step - 1, sub].wait_recv()
            value = value + z_in[way, step - 2, sub].astype(F32)
        z_out[way, step - 1, sub] = value.astype(BF16)
        copy = send(
            z_out.at[way, step - 1, sub], z_in.at[way, step - 1, sub],
            z_send.at[way, step - 1, sub], z_recv.at[way, step - 1, sub],
            up if way == 0 else down, h,
        )
        copy.start()
        z_copies[way, step, sub] = copy

    for sub, (t, half) in enumerate(SUBS):
        hop(t, 1, sub)
    for sub, (t, half) in enumerate(SUBS):
        hop(1 - t, 2, sub)

    d_copy.wait_recv()
    pair_out[...] = (dq_part[c, 1 - hp] + twin_in[1 - hp]).astype(BF16)
    y_copy = send(pair_out, pair_in, y_send.at[0], y_recv.at[0], s, pair)
    y_copy.start()

    for sub, (t, half) in enumerate(SUBS):
        hop(t, 2, sub)
    dq[...] = dq_part[c, hp] + twin_in[hp]
    for step in (3, 4):
        for sub in range(4):
            for way in range(2):
                hop(way, step, sub)

    a_copies = []
    for half in range(2):
        for t in range(2):
            sub = t * 2 + half
            value = dkv[t, rows_of(z, half), :]
            for way in range(2):
                z_copies[way, 4, sub].wait_recv()
                value = value + z_in[way, 3, sub].astype(F32)
            if t == 0:
                value = value * SCALE
            for k in range(4):
                fin[half * 4 + k, t] = value[k * TILE : (k + 1) * TILE, :]
        for k in range(4):
            seq, head, other = owners[half * 4 + k]
            g = x * 2 + y // 2
            copy = send(
                fin.at[half * 4 + k], own_in.at[g],
                a_send.at[half * 4 + k], a_recv.at[g], seq, head,
            )
            pl.when(other)(copy.start)
            a_copies.append((copy, other))

            @pl.when(jnp.logical_not(other))
            def _():
                own_in[g] = fin[half * 4 + k]

    y_copy.wait_recv()
    for g, (seq, head, other) in enumerate(makers):
        landed = send(fin.at[0], own_in.at[g], a_send.at[0], a_recv.at[g], seq, head)
        pl.when(other)(landed.wait_recv)

    for copy, other in a_copies:
        pl.when(other)(copy.wait_send)
    for copy in list(z_copies.values()) + [d_copy, y_copy]:
        copy.wait_send()


def scatter(dq_part, dkv):
    vmem = pl.BlockSpec(memory_space=pltpu.VMEM)
    dma = pltpu.SemaphoreType.DMA
    return pl.pallas_call(
        scatter_kernel,
        name="exchange_out",
        out_shape=(
            jax.ShapeDtypeStruct((ROWS, 2 * D), F32),
            jax.ShapeDtypeStruct((ROWS, 2 * D), BF16),
            jax.ShapeDtypeStruct((8, 2, TILE, D), F32),
        ),
        in_specs=[vmem] * 2,
        out_specs=(vmem,) * 3,
        scratch_shapes=[
            pltpu.VMEM((2, ROWS, 2 * D), F32),
            pltpu.VMEM((ROWS, 2 * D), BF16),
            pltpu.VMEM((2, 4, 4, HALF, D), BF16),
            pltpu.VMEM((2, 4, 4, HALF, D), BF16),
            pltpu.VMEM((8, 2, TILE, D), F32),
            dma((1,)), dma((1,)),
            dma((1,)), dma((1,)),
            dma((2, 4, 4)), dma((2, 4, 4)),
            dma((8,)), dma((8,)),
        ],
        compiler_params=pltpu.CompilerParams(collective_id=1, has_side_effects=True, vmem_limit_bytes=OUT_VMEM),
    )(dq_part, dkv)


def finish_kernel(sums, pair_in, own_in, dq, dk, dv):
    dq[...] = sums[...] + pair_in[...].astype(F32)
    for g in range(8):
        dk[:, g * D : (g + 1) * D] = own_in[g, 0]
        dv[:, g * D : (g + 1) * D] = own_in[g, 1]


def finish(sums, pair_in, own_in):
    vmem = pl.BlockSpec(memory_space=pltpu.VMEM)
    return pl.pallas_call(
        finish_kernel,
        name="finish",
        out_shape=(
            jax.ShapeDtypeStruct((ROWS, 2 * D), F32),
            jax.ShapeDtypeStruct((TILE, 8 * D), F32),
            jax.ShapeDtypeStruct((TILE, 8 * D), F32),
        ),
        in_specs=[vmem] * 3,
        out_specs=(vmem,) * 3,
        compiler_params=pltpu.CompilerParams(vmem_limit_bytes=8 * MIB),
    )(sums, pair_in, own_in)


def body(
    queries, keys, values, attn_out, out_grad, log_norm, block_layout, document_ids, block_order
):
    kv, q_all, g_all, s_all, l_all, below = gather(
        keys,
        values,
        queries,
        out_grad,
        attn_out,
        log_norm,
        block_layout,
        document_ids.reshape(NBLK, BLOCK),
    )
    dq_part, dkv = attend(
        block_order, below, kv.reshape(2, KEYS, D), q_all, g_all, s_all, l_all
    )
    return finish(*scatter(dq_part, dkv))


def solution(mesh):
    in_specs = (
        P("seq", "head"),
        P(("seq", "head"), None),
        P(("seq", "head"), None),
        P("seq", "head"),
        P("seq", "head"),
        P("head", "seq"),
        P("head", None, None),
        P(),
        P(),
    )
    out_specs = (P("seq", "head"), P(("seq", "head"), None), P(("seq", "head"), None))
    return jax.shard_map(body, mesh=mesh, in_specs=in_specs, out_specs=out_specs, check_vma=False)
```

```python
import jax
import jax.numpy as jnp
from jax import lax
from jax.experimental import pallas as pl
from jax.experimental.pallas import tpu as pltpu
from jax.sharding import PartitionSpec as P

MESH = pl.DeviceIdType.MESH
D = 128
BLOCK = 128
NBLK = 64
NZ = 8
TILE = 32
TILES = 8
PLANE = TILE * TILES
HALF = PLANE // 2
ROWS = 512
COLS = 512
BIG = 1e30
ALWAYS = 1 << 20
SCALE = D ** (-0.5)
LOG2E = 1.4426950408889634
BF16 = jnp.bfloat16
F32 = jnp.float32
NN = (((1,), (0,)), ((), ()))
NT = (((1,), (1,)), ((), ()))
TN = (((0,), (0,)), ((), ()))
AT_DOC = 64
AT_ONE = 72
SUBS = ((0, 0), (0, 1), (1, 0), (1, 1))
MIB = 1 << 20


def place():
    s = lax.axis_index("seq")
    h = lax.axis_index("head")
    return s, h, s // 2, s % 2, h // 4, h % 4


def send(src, dst, send_sem, recv_sem, seq, head):
    return pltpu.make_async_remote_copy(
        src_ref=src,
        dst_ref=dst,
        send_sem=send_sem,
        recv_sem=recv_sem,
        device_id=(seq, head),
        device_id_type=MESH,
    )


def dot(a, b, dims):
    return lax.dot_general(a, b, dims, preferred_element_type=F32)


def three(x):
    high = x.astype(BF16)
    rest = x - high.astype(F32)
    mid = rest.astype(BF16)
    low = (rest - mid.astype(F32)).astype(BF16)
    return [high, mid, low]


def iota(shape, dim):
    return lax.broadcasted_iota(jnp.int32, shape, dim)


def fused_kernel(
    keys_h, values_h, queries_h, grads_h, outs_h, norms_h, layout_h, ids_h, order_h, order,
    dq, pair_in, own_in,
    keys, values, queries, grads, outs, norms, layout, ids, order_v,
    kv, q_in, g_in, stats, s_in, lay, l_in, lperm, span,
    ax, qu, gu, qx, gx, acc, dqt, dqp, twin_in, pair_out, z_out, z_in, fin, ahead,
    l_sem, a_send, a_recv, k_send, k_recv, z_send, z_recv, y_send, y_recv, d_send, d_recv,
    f_send, f_recv, r_send, r_recv, b_send, b_recv,
):
    s, h, z, c, x, y = place()
    pair = h + 1 - 2 * (y % 2)
    twin = s + 1 - 2 * c
    up = ((z + 1) % NZ) * 2 + c
    down = ((z + NZ - 1) % NZ) * 2 + c
    hp = y % 2
    quarter = hp * 2 + c

    loads = []
    for i, (src, dst) in enumerate((
        (keys_h, keys), (values_h, values), (queries_h, queries), (grads_h, grads), (outs_h, outs),
        (norms_h, norms), (layout_h, layout), (ids_h, ids), (order_h, order_v),
    )):
        loads.append(pltpu.make_async_copy(src, dst, l_sem.at[i]))
        loads[i].start()

    takers, givers = [], []
    for xg in range(4):
        for yp in range(2):
            seq, head = z * 2 + y % 2, xg * 4 + yp * 2 + y // 2
            takers.append((seq, head, (seq != s) | (head != h)))
    for cg in range(2):
        for xg in range(4):
            seq, head = z * 2 + cg, xg * 4 + quarter
            givers.append((seq, head, (seq != s) | (head != h)))
    barrier = pltpu.get_barrier_semaphore()
    for seq, head in ((s, pair), (twin, h), (up, h), (down, h)):
        pl.semaphore_signal(barrier, inc=1, device_id=(seq, head), device_id_type=MESH)
    for seq, head, other in takers + givers:

        @pl.when(other)
        def _():
            pl.semaphore_signal(barrier, inc=1, device_id=(seq, head), device_id_type=MESH)

    own = ((y % 2 == c) & (y // 2 == hp)).astype(jnp.int32)
    acc[...] = jnp.zeros_like(acc)
    dqt[...] = jnp.zeros_like(dqt)
    for load in loads[:3]:
        load.wait()
    pl.semaphore_wait(barrier, 4 + 16 - 2 * own)

    slot = c * 4 + x
    slot_rows = pl.ds(pl.multiple_of(slot * TILE, TILE), TILE)
    a_copies = []
    for g, (seq, head, other) in enumerate(takers):
        for t, src in enumerate((keys, values)):
            copy = send(
                src.at[:, pl.ds(g * D, D)], kv.at[t, z, slot_rows, :],
                a_send.at[t, g], a_recv.at[t, slot], seq, head,
            )
            pl.when(other)(copy.start)
            a_copies.append((copy, other))

            @pl.when(jnp.logical_not(other))
            def _():
                kv[t, z, slot_rows, :] = src[:, g * D : (g + 1) * D]

    y_copies = [
        send(queries, q_in.at[1], y_send.at[0], y_recv.at[0], s, pair),
        send(grads, g_in.at[1], y_send.at[1], y_recv.at[1], s, pair),
        send(lay, l_in, y_send.at[2], y_recv.at[2], s, pair),
        send(stats, s_in.at[1], y_send.at[3], y_recv.at[3], s, pair),
    ]
    d_copies = [
        send(queries, q_in.at[0], d_send.at[0], d_recv.at[0], twin, h),
        send(grads, g_in.at[0], d_send.at[1], d_recv.at[1], twin, h),
        send(stats, s_in.at[0], d_send.at[2], d_recv.at[2], twin, h),
    ]
    y_copies[0].start()
    d_copies[0].start()
    for load in loads[3:]:
        load.wait()
    y_copies[1].start()
    d_copies[1].start()

    ones = jnp.ones((8, D), BF16)
    for hh in range(2):
        lay[hh * NBLK : (hh + 1) * NBLK, :] = layout[hh].astype(F32).astype(BF16)
        for rb in range(4):
            at = (slice(rb * BLOCK, (rb + 1) * BLOCK), slice(hh * D, (hh + 1) * D))
            product = grads[at].astype(F32) * outs[at].astype(F32)
            high = product.astype(BF16)
            low = (product - high.astype(F32)).astype(BF16)
            total = dot(ones, high, NT) + dot(ones, low, NT)
            stats[hh * 4 + rb : hh * 4 + rb + 1, :] = norms[hh : hh + 1, rb * BLOCK : (rb + 1) * BLOCK]
            stats[8 + hh * 4 + rb : 9 + hh * 4 + rb, :] = total[0:1, :]
    for copy in (y_copies[2], y_copies[3], d_copies[2]):
        copy.start()

    lane = iota((1, D), 1)
    first, after = jnp.zeros((1, D), F32), jnp.full((1, D), float(ALWAYS), F32)
    for d in range(1, 8):
        below = jnp.sum((ids[...] < d).astype(F32), axis=(0, 1), keepdims=True)
        first = jnp.where(lane == AT_DOC + d, below, first)
        after = jnp.where(lane == AT_DOC + d - 1, below, after)
    span[0:1, :] = first.astype(jnp.int32)
    span[1:2, :] = after.astype(jnp.int32)

    stored = (iota((NBLK, D), 0) == order_v[...]) & (iota((NBLK, D), 1) < NBLK)
    stored = stored.astype(F32).astype(BF16)
    lperm[0] = dot(lay[...], stored, NN)

    ahead[...] = quarter * TILE + iota((TILE, COLS), 0) - iota((TILE, COLS), 1) % BLOCK
    extra = (iota((8, D), 1) - AT_ONE == iota((8, D), 0)) & (iota((8, D), 0) < 3)
    extra = extra.astype(F32).astype(BF16)
    tile_lane = iota((1, D), 1) < NBLK
    doc_lane = (lane >= AT_DOC) & (lane < AT_ONE)

    def prepare(side, cb, q_piece, g_piece, s_piece):
        for rp in range(2):
            unit = cb * 2 + rp
            norm, delta = [], []
            for b in range(2):
                rb = rp * 2 + b
                for hh in range(2):
                    rows = pl.ds((b * 2 + hh) * BLOCK, BLOCK)
                    at = (slice(rb * BLOCK, (rb + 1) * BLOCK), slice(hh * D, (hh + 1) * D))
                    qu[side, unit, rows, :] = q_piece[at]
                    gu[side, unit, rows, :] = g_piece[at]
                    norm.append(s_piece[hh * 4 + rb : hh * 4 + rb + 1, :])
                    delta.append(s_piece[8 + hh * 4 + rb : 9 + hh * 4 + rb, :])
            zero = jnp.zeros((5, COLS), BF16)
            norm = jnp.concatenate(norm, axis=1) * (-1.0 / SCALE)
            delta = -jnp.concatenate(delta, axis=1)
            norm = dot(jnp.concatenate(three(norm) + [zero], axis=0), extra, TN)
            delta = dot(jnp.concatenate(three(delta) + [zero], axis=0), extra, TN)
            gx[side, unit] = delta.astype(BF16)
            for b in range(2):
                block = order[z * 8 + unit * 2 + b]
                position = block * BLOCK + iota((BLOCK, D), 0)
                apart = doc_lane & ((position < span[0:1, :]) | (position >= span[1:2, :]))
                for hh in range(2):
                    rows = pl.ds((b * 2 + hh) * BLOCK, BLOCK)
                    seen = lperm[side, pl.ds(hh * NBLK + block, 1), :]
                    hidden = tile_lane & ((seen < 0.5) | (order_v[...] > block))
                    base = norm[(b * 2 + hh) * BLOCK : (b * 2 + hh + 1) * BLOCK, :]
                    qx[side, unit, rows, :] = jnp.where(apart | hidden, -BIG, base).astype(BF16)

    def prepare_keys(plane):
        row, col = iota((TILE, D), 0), iota((TILE, D), 1)
        for t in range(TILES):
            position = order[plane * TILES + t] * BLOCK + quarter * TILE + row
            hot = col == plane * TILES + t
            hot = hot | (doc_lane & (position >= span[0:1, :]) & (position < span[1:2, :]))
            hot = hot | ((col >= AT_ONE) & (col < AT_ONE + 3))
            ax[plane, pl.ds(t * TILE, TILE), :] = hot.astype(F32).astype(BF16)

    def unit_grads(side, plane, unit):
        kc, vc, extra_k = kv[0, plane], kv[1, plane], ax[plane]
        q, g = qu[side, unit], gu[side, unit]
        scores = dot(jnp.concatenate([kc, extra_k], 1), jnp.concatenate([q, qx[side, unit]], 1), NT)
        grads_less = dot(jnp.concatenate([vc, extra_k], 1), jnp.concatenate([g, gx[side, unit]], 1), NT)
        low, score_grad = [], []
        for t in range(TILES):
            part = slice(t * TILE, (t + 1) * TILE)
            bound = []
            for b in range(2):
                same = order[plane * TILES + t] == order[z * 8 + unit * 2 + b]
                bound.append(jnp.full((1, 2 * BLOCK), jnp.where(same, 0, ALWAYS), jnp.int32))
            visible = ahead[...] <= jnp.concatenate(bound, axis=1)
            weights = jnp.where(visible, jnp.exp2(scores[part, :] * (SCALE * LOG2E)), 0.0)
            low.append(weights.astype(BF16))
            score_grad.append((weights * grads_less[part, :]).astype(BF16))
        low = jnp.concatenate(low, axis=0)
        score_grad = jnp.concatenate(score_grad, axis=0)
        acc[0, plane] += dot(score_grad, q, NN)
        acc[1, plane] += dot(low, g, NN)
        dqt[side, unit] += dot(kc, score_grad, TN)

    def compute(side, plane, units=(0, 4)):
        def one(unit, _):
            unit_grads(side, plane, unit)
            return 0

        lax.fori_loop(units[0], units[1], one, 0)

    def query_sums(side, cb):
        for rp in range(2):
            for b in range(2):
                for hh in range(2):
                    at = b * 2 + hh
                    block_grad = dqt[side, cb * 2 + rp, :, at * BLOCK : (at + 1) * BLOCK].T * SCALE
                    dqp[side, cb, (rp * 2 + b) * BLOCK : (rp * 2 + b + 1) * BLOCK, hh * D : (hh + 1) * D] = block_grad

    def hop_in(way, step, sub):
        t, half = SUBS[sub]
        origin = (z + NZ - (step - 1)) % NZ if way == 0 else (z + step - 1) % NZ
        piece = kv.at[t, origin, pl.ds(half * HALF, HALF), :]
        return send(
            piece, piece, k_send.at[way, step - 1, sub], k_recv.at[way, step - 1, sub],
            up if way == 0 else down, h,
        )

    def carries(way, step, sub):
        return step < 4 or (step == 4 and SUBS[sub][0] == way)

    k_copies = {}
    for sub, (t, half) in enumerate(SUBS):
        for k in range(4):
            at = half * 4 + k
            seq, head, other = givers[at]
            landed = send(
                keys.at[:, pl.ds(0, D)], kv.at[t, z, pl.ds(at * TILE, TILE), :],
                a_send.at[t, 0], a_recv.at[t, at], seq, head,
            )
            pl.when(other)(landed.wait_recv)
        for way in range(2):
            k_copies[way, 1, sub] = hop_in(way, 1, sub)
            k_copies[way, 1, sub].start()

    forwards = []

    def pass_on(k, ref):
        y_copies[k].wait_recv()
        i = len(forwards)
        copy = send(ref.at[1], ref.at[2], f_send.at[i], f_recv.at[i], twin, h)
        copy.start()
        forwards.append(copy)

    def arrive(step):
        for sub in range(4):
            for way in range(2):
                if carries(way, step, sub):
                    k_copies[way, step, sub].wait_recv()
                if carries(way, step + 1, sub):
                    k_copies[way, step + 1, sub] = hop_in(way, step + 1, sub)
                    k_copies[way, step + 1, sub].start()

    prepare(0, c, queries, grads, stats)
    for copy in d_copies:
        copy.wait_recv()
    prepare(0, 1 - c, q_in.at[0], g_in.at[0], s_in.at[0])
    prepare_keys(z)
    above = [(z + d) % NZ for d in range(5)]
    under = [(z + NZ - d) % NZ for d in range(4)]

    compute(0, z)
    arrive(1)
    for plane in (above[1], under[1]):
        prepare_keys(plane)
        compute(0, plane)
        if plane is above[1]:
            arrive(2)
    pass_on(0, q_in)
    for plane in (above[2], under[2]):
        prepare_keys(plane)
        compute(0, plane)
        if plane is above[2]:
            arrive(3)
    pass_on(1, g_in)
    pass_on(3, s_in)
    y_copies[2].wait_recv()
    lperm[1] = dot(l_in[...], stored, NN)
    for plane in (above[3], under[3]):
        prepare_keys(plane)
        compute(0, plane)
        if plane is above[3]:
            arrive(4)
    prepare_keys(above[4])
    compute(0, above[4])
    query_sums(0, 1 - c)
    own_copies = [send(dqp.at[0, 1 - c], twin_in.at[0], r_send.at[0], r_recv.at[0], twin, h)]
    own_copies[0].start()
    prepare(1, c, q_in.at[1], g_in.at[1], s_in.at[1])
    for copy in forwards:
        copy.wait_recv()
    prepare(1, 1 - c, q_in.at[2], g_in.at[2], s_in.at[2])

    z_copies = {}

    def hop_out(way, step, sub):
        t, half = SUBS[sub]
        target = (z + 5 - step) % NZ if way == 0 else (z + NZ - (5 - step)) % NZ
        value = acc[t, target, half * HALF : (half + 1) * HALF, :]
        if (way, step - 1, sub) in z_copies:
            z_copies[way, step - 1, sub].wait_recv()
            value = value + z_in[way, step - 2, sub].astype(F32)
        z_out[way, step - 1, sub] = value.astype(BF16)
        copy = send(
            z_out.at[way, step - 1, sub], z_in.at[way, step - 1, sub],
            z_send.at[way, step - 1, sub], z_recv.at[way, step - 1, sub],
            up if way == 0 else down, h,
        )
        copy.start()
        z_copies[way, step, sub] = copy

    compute(1, above[4])
    for sub in range(4):
        hop_out(SUBS[sub][0], 1, sub)
    for d in (3, 2, 1):
        for way in range(2):
            compute(1, above[d] if way == 0 else under[d])
            for sub in (2, 3, 0, 1) if way == 0 else (0, 1, 2, 3):
                hop_out(way, 5 - d, sub)
    compute(1, z, ((1 - c) * 2, (1 - c) * 2 + 2))
    query_sums(1, 1 - c)
    own_copies.append(send(dqp.at[1, 1 - c], twin_in.at[1], r_send.at[1], r_recv.at[1], twin, h))
    own_copies[1].start()
    compute(1, z, (c * 2, c * 2 + 2))
    query_sums(1, c)
    own_copies[1].wait_recv()
    pair_out[...] = (dqp[1, c] + twin_in[1]).astype(BF16)
    own_copies.append(send(pair_out, pair_in, r_send.at[2], r_recv.at[2], s, pair))
    own_copies[2].start()

    b_copies = []
    g = x * 2 + y // 2
    for half in range(2):
        for t in range(2):
            sub = t * 2 + half
            value = acc[t, z, half * HALF : (half + 1) * HALF, :]
            for way in range(2):
                z_copies[way, 4, sub].wait_recv()
                value = value + z_in[way, 3, sub].astype(F32)
            if t == 0:
                value = value * SCALE
            for k in range(4):
                fin[half * 4 + k, t] = value[k * TILE : (k + 1) * TILE, :]
        for k in range(4):
            seq, head, other = givers[half * 4 + k]
            copy = send(
                fin.at[half * 4 + k], own_in.at[g], b_send.at[half * 4 + k], b_recv.at[g], seq, head,
            )
            pl.when(other)(copy.start)
            b_copies.append((copy, other))

            @pl.when(jnp.logical_not(other))
            def _():
                own_in[g] = fin[half * 4 + k]

    query_sums(0, c)
    own_copies[0].wait_recv()
    dq[...] = dqp[0, c] + twin_in[0]

    for g, (seq, head, other) in enumerate(takers):
        landed = send(fin.at[0], own_in.at[g], b_send.at[0], b_recv.at[g], seq, head)
        pl.when(other)(landed.wait_recv)
    own_copies[2].wait_recv()

    for copy, other in a_copies + b_copies:
        pl.when(other)(copy.wait_send)
    for copy in list(k_copies.values()) + list(z_copies.values()):
        copy.wait_send()
    for copy in y_copies + d_copies + forwards + own_copies:
        copy.wait_send()


def fused(keys, values, queries, grads, outs, norms, layout, ids, order):
    vmem = pl.BlockSpec(memory_space=pltpu.VMEM)
    smem = pl.BlockSpec(memory_space=pltpu.SMEM)
    hbm = pl.BlockSpec(memory_space=pltpu.HBM)
    dma = pltpu.SemaphoreType.DMA
    v = pltpu.VMEM
    return pl.pallas_call(
        fused_kernel,
        name="fused",
        out_shape=(
            jax.ShapeDtypeStruct((ROWS, 2 * D), F32),
            jax.ShapeDtypeStruct((ROWS, 2 * D), BF16),
            jax.ShapeDtypeStruct((8, 2, TILE, D), F32),
        ),
        in_specs=[hbm] * 9 + [smem],
        out_specs=(vmem,) * 3,
        scratch_shapes=[
            v((TILE, 8 * D), BF16), v((TILE, 8 * D), BF16),
            v((ROWS, 2 * D), BF16), v((ROWS, 2 * D), BF16), v((ROWS, 2 * D), BF16),
            v((2, ROWS), F32), v((2, NBLK, NBLK), jnp.int32),
            v((NBLK, BLOCK), jnp.int32), v((1, D), jnp.int32),
            v((2, NZ, PLANE, D), BF16),
            v((3, ROWS, 2 * D), BF16), v((3, ROWS, 2 * D), BF16),
            v((16, BLOCK), F32), v((3, 16, BLOCK), F32),
            v((2 * NBLK, NBLK), BF16), v((2 * NBLK, NBLK), BF16),
            v((2, 2 * NBLK, D), F32), v((8, D), jnp.int32),
            v((NZ, PLANE, D), BF16),
            v((2, 4, COLS, D), BF16), v((2, 4, COLS, D), BF16),
            v((2, 4, COLS, D), BF16), v((2, 4, COLS, D), BF16),
            v((2, NZ, PLANE, D), F32),
            v((2, 4, D, COLS), F32),
            v((2, 2, ROWS, 2 * D), F32),
            v((2, ROWS, 2 * D), F32), v((ROWS, 2 * D), BF16),
            v((2, 4, 4, HALF, D), BF16), v((2, 4, 4, HALF, D), BF16),
            v((8, 2, TILE, D), F32),
            v((TILE, COLS), jnp.int32),
            dma((9,)), dma((2, 8)), dma((2, 8)),
            dma((2, 4, 4)), dma((2, 4, 4)), dma((2, 4, 4)), dma((2, 4, 4)),
            dma((4,)), dma((4,)), dma((3,)), dma((3,)),
            dma((3,)), dma((3,)), dma((3,)), dma((3,)), dma((8,)), dma((8,)),
        ],
        compiler_params=pltpu.CompilerParams(
            collective_id=0, has_side_effects=True, vmem_limit_bytes=40 * MIB
        ),
    )(keys, values, queries, grads, outs, norms, layout, ids, jnp.pad(order, (0, D - NBLK)).reshape(1, D), order)


def finish_kernel(sums, pair_in, own_in, dq, dk, dv):
    dq[...] = sums[...] + pair_in[...].astype(F32)
    for g in range(8):
        dk[:, g * D : (g + 1) * D] = own_in[g, 0]
        dv[:, g * D : (g + 1) * D] = own_in[g, 1]


def finish(sums, pair_in, own_in):
    vmem = pl.BlockSpec(memory_space=pltpu.VMEM)
    return pl.pallas_call(
        finish_kernel,
        name="finish",
        out_shape=(
            jax.ShapeDtypeStruct((ROWS, 2 * D), F32),
            jax.ShapeDtypeStruct((TILE, 8 * D), F32),
            jax.ShapeDtypeStruct((TILE, 8 * D), F32),
        ),
        in_specs=[vmem] * 3,
        out_specs=(vmem,) * 3,
        compiler_params=pltpu.CompilerParams(vmem_limit_bytes=8 * MIB),
    )(sums, pair_in, own_in)


def body(
    queries, keys, values, attn_out, out_grad, log_norm, block_layout, document_ids, block_order
):
    return finish(
        *fused(
            keys,
            values,
            queries,
            out_grad,
            attn_out,
            log_norm,
            block_layout,
            document_ids.reshape(NBLK, BLOCK),
            block_order,
        )
    )


def solution(mesh):
    in_specs = (
        P("seq", "head"),
        P(("seq", "head"), None),
        P(("seq", "head"), None),
        P("seq", "head"),
        P("seq", "head"),
        P("head", "seq"),
        P("head", None, None),
        P(),
        P(),
    )
    out_specs = (P("seq", "head"), P(("seq", "head"), None), P(("seq", "head"), None))
    return jax.shard_map(body, mesh=mesh, in_specs=in_specs, out_specs=out_specs, check_vma=False)
```

```python
import jax
import jax.numpy as jnp
from jax import lax
from jax.experimental import pallas as pl
from jax.experimental.pallas import tpu as pltpu
from jax.sharding import PartitionSpec as P

MESH = pl.DeviceIdType.MESH
D = 128
BLOCK = 128
NBLK = 64
NZ = 8
TILE = 32
TILES = 8
PLANE = TILE * TILES
ROWS = 512
COLS = 512
BIG = 1e30
ALWAYS = 1 << 20
SCALE = D ** (-0.5)
LOG2E = 1.4426950408889634
BF16 = jnp.bfloat16
F32 = jnp.float32
NN = (((1,), (0,)), ((), ()))
NT = (((1,), (1,)), ((), ()))
TN = (((0,), (0,)), ((), ()))
AT_DOC = 64
AT_ONE = 72
MIB = 1 << 20


def place():
    s = lax.axis_index("seq")
    h = lax.axis_index("head")
    return s, h, s // 2, s % 2, h // 4, h % 4


def send(src, dst, send_sem, recv_sem, seq, head):
    return pltpu.make_async_remote_copy(
        src_ref=src,
        dst_ref=dst,
        send_sem=send_sem,
        recv_sem=recv_sem,
        device_id=(seq, head),
        device_id_type=MESH,
    )


def dot(a, b, dims):
    return lax.dot_general(a, b, dims, preferred_element_type=F32)


def three(x):
    high = x.astype(BF16)
    rest = x - high.astype(F32)
    mid = rest.astype(BF16)
    low = (rest - mid.astype(F32)).astype(BF16)
    return [high, mid, low]


def iota(shape, dim):
    return lax.broadcasted_iota(jnp.int32, shape, dim)


def fused_kernel(
    keys_h, values_h, queries_h, grads_h, outs_h, norms_h, layout_h, ids_h, order_h,
    dq, pair_in, own_in,
    keys, values, queries, grads, outs, norms, layout, ids, order, order_v,
    kv, qt, gt, st, lay, l_in, lperm, spans, docs,
    ax, qx, gx, lows, sgs, acc, dqt, dqp, twin_in, pair_out, z_out, z_in, fin, ahead, pick,
    l_sem, a_send, a_recv, k_send, k_recv, z_send, z_recv, y_send, y_recv, d_send, d_recv,
    f_send, f_recv, r_send, r_recv, b_send, b_recv,
):
    s, h, z, c, x, y = place()
    pair = h + 1 - 2 * (y % 2)
    twin = s + 1 - 2 * c
    up = ((z + 1) % NZ) * 2 + c
    down = ((z + NZ - 1) % NZ) * 2 + c
    hp = y % 2
    quarter = hp * 2 + c

    loads = []
    for i, (src, dst) in enumerate((
        (queries_h, queries), (keys_h, keys), (values_h, values), (grads_h, grads), (outs_h, outs),
        (norms_h, norms), (layout_h, layout), (ids_h, ids), (order_h, order),
    )):
        loads.append(pltpu.make_async_copy(src, dst, l_sem.at[i]))
        loads[i].start()

    takers, givers = [], []
    for xg in range(4):
        for yp in range(2):
            seq, head = z * 2 + y % 2, xg * 4 + yp * 2 + y // 2
            takers.append((seq, head, (seq != s) | (head != h)))
    for cg in range(2):
        for xg in range(4):
            seq, head = z * 2 + cg, xg * 4 + quarter
            givers.append((seq, head, (seq != s) | (head != h)))
    barrier = pltpu.get_barrier_semaphore()
    for seq, head in ((s, pair), (twin, h), (up, h), (down, h)):
        pl.semaphore_signal(barrier, inc=1, device_id=(seq, head), device_id_type=MESH)
    for seq, head, other in takers + givers:

        @pl.when(other)
        def _():
            pl.semaphore_signal(barrier, inc=1, device_id=(seq, head), device_id_type=MESH)

    above = [(z + d) % NZ for d in range(5)]
    under = [(z + NZ - d) % NZ for d in range(5)]
    own = ((y % 2 == c) & (y // 2 == hp)).astype(jnp.int32)
    mine = pl.ds(c * 2, 2)

    def columns(source, target):
        for rb in range(4):
            for hh in range(2):
                at = (rb % 2 * 2 + hh) * BLOCK
                block = source[rb * BLOCK : (rb + 1) * BLOCK, hh * D : (hh + 1) * D]
                target[0, c * 2 + rb // 2, :, at : at + BLOCK] = block.T

    loads[0].wait()
    columns(queries, qt)
    for load in loads[1:4]:
        load.wait()
    columns(grads, gt)
    pl.semaphore_wait(barrier, 4 + 16 - 2 * own)

    slot = c * 4 + x
    slot_rows = pl.ds(pl.multiple_of(slot * TILE, TILE), TILE)
    a_copies = []
    for t, src in enumerate((keys, values)):
        for g, (seq, head, other) in enumerate(takers):
            copy = send(
                src.at[:, pl.ds(g * D, D)], kv.at[t, z, slot_rows, :],
                a_send.at[t, g], a_recv.at[t, slot], seq, head,
            )
            pl.when(other)(copy.start)
            a_copies.append((copy, other))

            @pl.when(jnp.logical_not(other))
            def _():
                kv[t, z, slot_rows, :] = src[:, g * D : (g + 1) * D]

    def y_copy(k):
        src = (qt.at[0, mine], gt.at[0, mine], lay, st.at[0, c])[k]
        dst = (qt.at[1, mine], gt.at[1, mine], l_in, st.at[1, c])[k]
        return send(src, dst, y_send.at[k], y_recv.at[k], s, pair)

    d_copies = [
        send(qt.at[0, mine], qt.at[0, mine], d_send.at[0], d_recv.at[0], twin, h),
        send(gt.at[0, mine], gt.at[0, mine], d_send.at[1], d_recv.at[1], twin, h),
        send(st.at[0, c], st.at[0, c], d_send.at[2], d_recv.at[2], twin, h),
    ]
    for copy in (y_copy(0), d_copies[0], d_copies[1], y_copy(1)):
        copy.start()
    for load in loads[4:]:
        load.wait()

    ones = jnp.ones((8, D), BF16)
    for hh in range(2):
        lay[hh * NBLK : (hh + 1) * NBLK, :] = layout[hh].astype(F32).astype(BF16)
        for rb in range(4):
            at = (slice(rb * BLOCK, (rb + 1) * BLOCK), slice(hh * D, (hh + 1) * D))
            product = grads[at].astype(F32) * outs[at].astype(F32)
            high = product.astype(BF16)
            low = (product - high.astype(F32)).astype(BF16)
            total = dot(ones, high, NT) + dot(ones, low, NT)
            row = hh * 4 + rb
            st[0, c, row : row + 1, :] = norms[hh : hh + 1, rb * BLOCK : (rb + 1) * BLOCK]
            st[0, c, 8 + row : 9 + row, :] = total[0:1, :]
    for copy in (y_copy(3), d_copies[2], y_copy(2)):
        copy.start()
    acc[...] = jnp.zeros_like(acc)
    dqt[...] = jnp.zeros_like(dqt)
    qx[...] = jnp.zeros_like(qx)
    gx[...] = jnp.zeros_like(gx)
    pick[...] = jnp.zeros_like(pick)

    lane = iota((1, D), 1)
    placed = jnp.zeros((1, D), jnp.int32)
    for sb in range(NBLK):
        placed = jnp.where(lane == sb, order[sb], placed)
    order_v[...] = placed
    first, after = jnp.zeros((1, D), F32), jnp.full((1, D), float(ALWAYS), F32)
    row8 = iota((8, COLS), 0)
    first_row, after_row = jnp.zeros((8, COLS), F32), jnp.full((8, COLS), float(ALWAYS), F32)
    for d in range(1, 8):
        below = jnp.sum((ids[...] < d).astype(F32), axis=(0, 1), keepdims=True)
        first = jnp.where(lane == AT_DOC + d, below, first)
        after = jnp.where(lane == AT_DOC + d - 1, below, after)
        first_row = jnp.where(row8 == d, below, first_row)
        after_row = jnp.where(row8 == d - 1, below, after_row)
    spans[0:1, :] = first.astype(jnp.int32)
    spans[1:2, :] = after.astype(jnp.int32)
    docs[0] = first_row.astype(jnp.int32)
    docs[1] = after_row.astype(jnp.int32)

    stored = (iota((NBLK, D), 0) == order_v[...]) & (iota((NBLK, D), 1) < NBLK)
    stored = stored.astype(F32).astype(BF16)
    lperm[0] = dot(lay[...], stored, NN)
    ahead[...] = quarter * TILE + iota((TILE, COLS), 0) - iota((TILE, COLS), 1) % BLOCK
    spread = (iota((8, COLS), 1) // BLOCK == iota((8, COLS), 0)).astype(F32)
    doc_lane = (lane >= AT_DOC) & (lane < AT_ONE)

    def prepare(side, cb):
        for rp in range(2):
            unit = cb * 2 + rp
            norm, delta, position = [], [], []
            for b in range(2):
                block = order[z * 8 + unit * 2 + b]
                for hh in range(2):
                    at, row = b * 2 + hh, hh * 4 + rp * 2 + b
                    norm.append(st[side, cb, row : row + 1, :])
                    delta.append(st[side, cb, 8 + row : 9 + row, :])
                    position.append(block * BLOCK + iota((1, BLOCK), 1))
                    seen = lperm[side, pl.ds(hh * NBLK + block, 1), :]
                    pick[at : at + 1, :] = jnp.where((seen > 0.5) & (order_v[...] <= block), 1.0, 0.0)
            norm = three(jnp.concatenate(norm, axis=1) * (-1.0 / SCALE))
            delta = three(-jnp.concatenate(delta, axis=1))
            position = jnp.concatenate(position, axis=1)
            seen = dot(pick[...], spread, TN)
            qx[side, unit, 0:NBLK, :] = jnp.where(seen[0:NBLK, :] > 0.5, 0.0, -BIG).astype(BF16)
            inside = (position >= docs[0]) & (position < docs[1])
            zero = jnp.zeros((8, COLS), F32)
            for ref, rows, head in ((qx, norm, jnp.where(inside, 0.0, -BIG)), (gx, delta, zero)):
                parts = zero
                for i in range(3):
                    parts = jnp.where(row8 == i, rows[i].astype(F32), parts)
                ref[side, unit, AT_DOC : AT_DOC + 16, :] = jnp.concatenate([head, parts], axis=0).astype(BF16)

    def prepare_keys(plane):
        row, col = iota((TILE, D), 0), iota((TILE, D), 1)
        for t in range(TILES):
            position = order[plane * TILES + t] * BLOCK + quarter * TILE + row
            hot = col == plane * TILES + t
            hot = hot | (doc_lane & (position >= spans[0:1, :]) & (position < spans[1:2, :]))
            hot = hot | ((col >= AT_ONE) & (col < AT_ONE + 3))
            ax[plane, pl.ds(t * TILE, TILE), :] = hot.astype(F32).astype(BF16)

    def spot(n):
        side = n // 32
        j = n % 32 // 4
        j = j + side * (7 - 2 * j)
        away = (j + 1) // 2
        return (z + NZ + away * (1 - 2 * (j % 2))) % NZ, side, n % 4

    def front(n):
        plane, side, unit = spot(n)
        extra = ax[plane]
        scores = dot(
            jnp.concatenate([kv[0, plane], extra], 1), jnp.concatenate([qt[side, unit], qx[side, unit]], 0), NN
        )
        grads_less = dot(
            jnp.concatenate([kv[1, plane], extra], 1), jnp.concatenate([gt[side, unit], gx[side, unit]], 0), NN
        )
        low, score_grad = [], []
        for t in range(TILES):
            part = slice(t * TILE, (t + 1) * TILE)
            bound = []
            for b in range(2):
                same = order[plane * TILES + t] == order[z * 8 + unit * 2 + b]
                bound.append(jnp.full((1, 2 * BLOCK), jnp.where(same, 0, ALWAYS), jnp.int32))
            visible = ahead[...] <= jnp.concatenate(bound, axis=1)
            weights = jnp.where(visible, jnp.exp2(scores[part, :] * (SCALE * LOG2E)), 0.0)
            low.append(weights.astype(BF16))
            score_grad.append((weights * grads_less[part, :]).astype(BF16))
        return jnp.concatenate(low, axis=0), jnp.concatenate(score_grad, axis=0)

    def back(n, low, score_grad):
        plane, side, unit = spot(n)
        acc[0, plane] += dot(qt[side, unit], score_grad, NT)
        acc[1, plane] += dot(gt[side, unit], low, NT)
        dqt[side, unit] += dot(kv[0, plane], score_grad, TN)

    def query_sums(side, cb):
        for rb in range(4):
            for hh in range(2):
                at = (rb % 2 * 2 + hh) * BLOCK
                block_grad = dqt[side, cb * 2 + rb // 2, :, at : at + BLOCK].T * SCALE
                dqp[side, cb, rb * BLOCK : (rb + 1) * BLOCK, hh * D : (hh + 1) * D] = block_grad

    def key_copy(way, step, t):
        piece = kv.at[t, under[step - 1] if way == 0 else above[step - 1]]
        return send(
            piece, piece, k_send.at[way, step - 1, t], k_recv.at[way, step - 1, t],
            up if way == 0 else down, h,
        )

    def carries(way, step, t):
        return step < 4 or (step == 4 and t == way)

    def arrive(step, t):
        for way in range(2):
            if carries(way, step, t):
                key_copy(way, step, t).wait_recv()
            if carries(way, step + 1, t):
                key_copy(way, step + 1, t).start()

    for t in range(2):
        for at, (seq, head, other) in enumerate(givers):
            landed = send(
                keys.at[:, pl.ds(0, D)], kv.at[t, z, pl.ds(at * TILE, TILE), :],
                a_send.at[t, 0], a_recv.at[t, at], seq, head,
            )
            pl.when(other)(landed.wait_recv)
        for way in range(2):
            key_copy(way, 1, t).start()

    def forward(k):
        src = (qt.at[1, mine], gt.at[1, mine], None, st.at[1, c])[k]
        return send(src, src, f_send.at[k], f_recv.at[k], twin, h)

    def pass_on(k):
        y_copy(k).wait_recv()
        forward(k).start()

    def sum_copy(way, step, t):
        return send(
            z_out.at[way, step - 1, t], z_in.at[way, step - 1, t],
            z_send.at[way, step - 1, t], z_recv.at[way, step - 1, t],
            up if way == 0 else down, h,
        )

    def pass_sum(way, step, t):
        value = acc[t, (above if way == 0 else under)[5 - step]]
        if step > 2 or (step == 2 and t == way):
            sum_copy(way, step - 1, t).wait_recv()
            value = value + z_in[way, step - 2, t].astype(F32)
        z_out[way, step - 1, t] = value.astype(BF16)
        sum_copy(way, step, t).start()

    def twin_copy(side):
        return send(dqp.at[side, 1 - c], twin_in.at[side], r_send.at[side], r_recv.at[side], twin, h)

    def twin_sums(side):
        query_sums(side, 1 - c)
        twin_copy(side).start()

    prepare(0, c)
    prepare_keys(z)
    for copy in d_copies:
        copy.wait_recv()
    prepare(0, 1 - c)
    lows[0], sgs[0] = front(0)

    def planes_at(away):
        prepare_keys(under[away])
        if away < 4:
            prepare_keys(above[away])

    def heads_come():
        pass_on(1)
        pass_on(3)
        y_copy(2).wait_recv()

    def other_heads():
        lperm[1] = dot(l_in[...], stored, NN)
        prepare(1, c)
        for k in (0, 1, 3):
            forward(k).wait_recv()
        prepare(1, 1 - c)

    def sums(*which):
        for w in which:
            pass_sum(*w)

    events = {
        1: lambda: (planes_at(1), arrive(1, 0), arrive(1, 1)),
        3: lambda: (planes_at(2), arrive(2, 0), pass_on(0)),
        5: lambda: arrive(2, 1),
        7: lambda: (planes_at(3), arrive(3, 0)),
        9: lambda: (arrive(3, 1), heads_come()),
        11: lambda: (planes_at(4), arrive(4, 0)),
        13: lambda: (other_heads(), arrive(4, 1)),
        21: lambda: twin_sums(0),
        18: lambda: sums((0, 1, 0), (1, 1, 1)),
        20: lambda: sums((0, 2, 1)),
        22: lambda: sums((1, 2, 0)),
        24: lambda: sums((0, 2, 0), (1, 2, 1)),
        26: lambda: sums((0, 3, 1)),
        28: lambda: sums((1, 3, 0)),
        30: lambda: sums((0, 3, 0), (1, 3, 1)),
    }

    def two(i, _):
        for at, event in events.items():
            pl.when(i == at)(lambda event=event: (event(), None)[1])
        n = 2 * i
        lows[1], sgs[1] = front(n + 1)
        back(n, lows[0], sgs[0])
        lows[0], sgs[0] = front(jnp.minimum(n + 2, 63))
        back(n + 1, lows[1], sgs[1])
        return 0

    lax.fori_loop(0, 32, two, 0)

    twin_sums(1)
    sums((0, 4, 1), (1, 4, 0))
    query_sums(1, c)
    twin_copy(1).wait_recv()
    pair_out[...] = (dqp[1, c] + twin_in[1]).astype(BF16)
    pair_copy = send(pair_out, pair_in, r_send.at[2], r_recv.at[2], s, pair)
    pair_copy.start()
    sums((0, 4, 0), (1, 4, 1))
    query_sums(0, c)
    twin_copy(0).wait_recv()
    dq[...] = dqp[0, c] + twin_in[0]

    b_copies = []
    g = x * 2 + y // 2
    for t in (1, 0):
        value = acc[t, z]
        for way in (0, 1):
            sum_copy(way, 4, t).wait_recv()
            value = value + z_in[way, 3, t].astype(F32)
        if t == 0:
            value = value * SCALE
        value = value.T
        for k in range(8):
            fin[k, t] = value[k * TILE : (k + 1) * TILE, :]
    for k, (seq, head, other) in enumerate(givers):
        copy = send(fin.at[k], own_in.at[g], b_send.at[k], b_recv.at[g], seq, head)
        pl.when(other)(copy.start)
        b_copies.append((copy, other))

        @pl.when(jnp.logical_not(other))
        def _():
            own_in[g] = fin[k]

    for g, (seq, head, other) in enumerate(takers):
        landed = send(fin.at[0], own_in.at[g], b_send.at[0], b_recv.at[g], seq, head)
        pl.when(other)(landed.wait_recv)
    pair_copy.wait_recv()

    for copy, other in a_copies + b_copies:
        pl.when(other)(copy.wait_send)
    for way in range(2):
        for t in range(2):
            for step in range(1, 5):
                if carries(way, step, t):
                    key_copy(way, step, t).wait_send()
                if step > 1 or t == way:
                    sum_copy(way, step, t).wait_send()
    for k in range(4):
        y_copy(k).wait_send()
        if k != 2:
            forward(k).wait_send()
    for copy in d_copies + [twin_copy(0), twin_copy(1), pair_copy]:
        copy.wait_send()


def fused(keys, values, queries, grads, outs, norms, layout, ids, order):
    vmem = pl.BlockSpec(memory_space=pltpu.VMEM)
    hbm = pl.BlockSpec(memory_space=pltpu.HBM)
    dma = pltpu.SemaphoreType.DMA
    v = pltpu.VMEM
    return pl.pallas_call(
        fused_kernel,
        name="fused",
        out_shape=(
            jax.ShapeDtypeStruct((ROWS, 2 * D), F32),
            jax.ShapeDtypeStruct((ROWS, 2 * D), BF16),
            jax.ShapeDtypeStruct((8, 2, TILE, D), F32),
        ),
        in_specs=[hbm] * 9,
        out_specs=(vmem,) * 3,
        scratch_shapes=[
            v((TILE, 8 * D), BF16), v((TILE, 8 * D), BF16),
            v((ROWS, 2 * D), BF16), v((ROWS, 2 * D), BF16), v((ROWS, 2 * D), BF16),
            v((2, ROWS), F32), v((2, NBLK, NBLK), jnp.int32),
            v((NBLK, BLOCK), jnp.int32), pltpu.SMEM((NBLK,), jnp.int32), v((1, D), jnp.int32),
            v((2, NZ, PLANE, D), BF16),
            v((2, 4, D, COLS), BF16), v((2, 4, D, COLS), BF16),
            v((2, 2, 16, BLOCK), F32),
            v((2 * NBLK, NBLK), BF16), v((2 * NBLK, NBLK), BF16),
            v((2, 2 * NBLK, D), F32), v((8, D), jnp.int32), v((2, 8, COLS), jnp.int32),
            v((NZ, PLANE, D), BF16),
            v((2, 4, D, COLS), BF16), v((2, 4, D, COLS), BF16),
            v((2, PLANE, COLS), BF16), v((2, PLANE, COLS), BF16),
            v((2, NZ, D, PLANE), F32),
            v((2, 4, D, COLS), F32),
            v((2, 2, ROWS, 2 * D), F32),
            v((2, ROWS, 2 * D), F32), v((ROWS, 2 * D), BF16),
            v((2, 4, 2, D, PLANE), BF16), v((2, 4, 2, D, PLANE), BF16),
            v((8, 2, TILE, D), F32),
            v((TILE, COLS), jnp.int32), v((8, D), F32),
            dma((9,)), dma((2, 8)), dma((2, 8)),
            dma((2, 4, 2)), dma((2, 4, 2)), dma((2, 4, 2)), dma((2, 4, 2)),
            dma((4,)), dma((4,)), dma((3,)), dma((3,)),
            dma((4,)), dma((4,)), dma((3,)), dma((3,)), dma((8,)), dma((8,)),
        ],
        compiler_params=pltpu.CompilerParams(
            collective_id=0, has_side_effects=True, vmem_limit_bytes=60 * MIB
        ),
    )(keys, values, queries, grads, outs, norms, layout, ids, order)


def finish_kernel(sums, pair_in, own_in, dq, dk, dv):
    dq[...] = sums[...] + pair_in[...].astype(F32)
    for g in range(8):
        dk[:, g * D : (g + 1) * D] = own_in[g, 0]
        dv[:, g * D : (g + 1) * D] = own_in[g, 1]


def finish(sums, pair_in, own_in):
    vmem = pl.BlockSpec(memory_space=pltpu.VMEM)
    return pl.pallas_call(
        finish_kernel,
        name="finish",
        out_shape=(
            jax.ShapeDtypeStruct((ROWS, 2 * D), F32),
            jax.ShapeDtypeStruct((TILE, 8 * D), F32),
            jax.ShapeDtypeStruct((TILE, 8 * D), F32),
        ),
        in_specs=[vmem] * 3,
        out_specs=(vmem,) * 3,
        compiler_params=pltpu.CompilerParams(vmem_limit_bytes=60 * MIB),
    )(sums, pair_in, own_in)


def body(
    queries, keys, values, attn_out, out_grad, log_norm, block_layout, document_ids, block_order
):
    return finish(
        *fused(
            keys,
            values,
            queries,
            out_grad,
            attn_out,
            log_norm,
            block_layout,
            document_ids.reshape(NBLK, BLOCK),
            block_order,
        )
    )


def solution(mesh):
    in_specs = (
        P("seq", "head"),
        P(("seq", "head"), None),
        P(("seq", "head"), None),
        P("seq", "head"),
        P("seq", "head"),
        P("head", "seq"),
        P("head", None, None),
        P(),
        P(),
    )
    out_specs = (P("seq", "head"), P(("seq", "head"), None), P(("seq", "head"), None))
    return jax.shard_map(body, mesh=mesh, in_specs=in_specs, out_specs=out_specs, check_vma=False)
```

```python
import jax
import jax.numpy as jnp
from jax import lax
from jax.experimental import pallas as pl
from jax.experimental.pallas import tpu as pltpu
from jax.sharding import PartitionSpec as P

MESH = pl.DeviceIdType.MESH
D = 128
BLOCK = 128
NBLK = 64
NZ = 8
TILE = 32
TILES = 8
PLANE = TILE * TILES
ROWS = 512
COLS = 512
BIG = 1e30
ALWAYS = 1 << 20
SCALE = D ** (-0.5)
LOG2E = 1.4426950408889634
BF16 = jnp.bfloat16
F32 = jnp.float32
NN = (((1,), (0,)), ((), ()))
NT = (((1,), (1,)), ((), ()))
TN = (((0,), (0,)), ((), ()))
AT_DOC = 64
AT_ONE = 72
MIB = 1 << 20


def place():
    s = lax.axis_index("seq")
    h = lax.axis_index("head")
    return s, h, s // 2, s % 2, h // 4, h % 4


def send(src, dst, send_sem, recv_sem, seq, head):
    return pltpu.make_async_remote_copy(
        src_ref=src,
        dst_ref=dst,
        send_sem=send_sem,
        recv_sem=recv_sem,
        device_id=(seq, head),
        device_id_type=MESH,
    )


def dot(a, b, dims):
    return lax.dot_general(a, b, dims, preferred_element_type=F32)


def three(x):
    high = x.astype(BF16)
    rest = x - high.astype(F32)
    mid = rest.astype(BF16)
    low = (rest - mid.astype(F32)).astype(BF16)
    return [high, mid, low]


def iota(shape, dim):
    return lax.broadcasted_iota(jnp.int32, shape, dim)


def fused_kernel(
    keys_h, values_h, queries_h, grads_h, outs_h, norms_h, layout_h, ids_h, order_h,
    dq, pair_in, own_in, way_in,
    keys, values, queries, grads, outs, norms, layout, ids, order, order_v,
    kv, qt, gt, st, lay, l_in, lperm, spans, docs,
    ax, qx, gx, lows, sgs, acc, dqt, dqp, twin_in, pair_out, z_out, z_in, fin, fin_way, ahead, pick,
    l_sem, a_send, a_recv, k_send, k_recv, z_send, z_recv, y_send, y_recv, d_send, d_recv,
    f_send, f_recv, r_send, r_recv, b_send, b_recv, w_send, w_recv,
):
    s, h, z, c, x, y = place()
    pair = h + 1 - 2 * (y % 2)
    twin = s + 1 - 2 * c
    up = ((z + 1) % NZ) * 2 + c
    down = ((z + NZ - 1) % NZ) * 2 + c
    hp = y % 2
    inner = (y + 1) // 2 % 2
    quarter = inner + c * (3 - 2 * inner)

    loads = []
    for i, (src, dst) in enumerate((
        (queries_h, queries), (keys_h, keys), (values_h, values), (grads_h, grads), (outs_h, outs),
        (norms_h, norms), (layout_h, layout), (ids_h, ids), (order_h, order),
    )):
        loads.append(pltpu.make_async_copy(src, dst, l_sem.at[i]))
        loads[i].start()

    above = [(z + d) % NZ for d in range(5)]
    under = [(z + NZ - d) % NZ for d in range(5)]
    own = (y // 2 == c).astype(jnp.int32)

    def takers(plane):
        out = []
        for xg in range(4):
            for yp in range(2):
                head = xg * 4 + (inner if yp == 0 else 3 - inner)
                out.append((plane * 2 + y // 2, head, (plane * 2 + y // 2 != s) | (head != h)))
        return out

    def givers(plane):
        out = []
        for cg in range(2):
            for xg in range(4):
                seq, head = plane * 2 + cg, xg * 4 + quarter
                out.append((seq, head, (seq != s) | (head != h)))
        return out

    near = (z, above[1], under[1])
    barrier = pltpu.get_barrier_semaphore()
    for seq, head in ((s, pair), (twin, h), (up, h), (down, h)):
        pl.semaphore_signal(barrier, inc=1, device_id=(seq, head), device_id_type=MESH)
    for plane in near:
        for seq, head, other in takers(plane) + givers(plane):

            @pl.when(other)
            def _():
                pl.semaphore_signal(barrier, inc=1, device_id=(seq, head), device_id_type=MESH)

    mine = pl.ds(c * 2, 2)

    def columns(source, target):
        for rb in range(4):
            for hh in range(2):
                at = (rb % 2 * 2 + hh) * BLOCK
                block = source[rb * BLOCK : (rb + 1) * BLOCK, hh * D : (hh + 1) * D]
                target[0, c * 2 + rb // 2, :, at : at + BLOCK] = block.T

    loads[0].wait()
    columns(queries, qt)
    for load in loads[1:4]:
        load.wait()
    columns(grads, gt)
    pl.semaphore_wait(barrier, 4 + 48 - 2 * own)

    slot = c * 4 + x
    slot_rows = pl.ds(pl.multiple_of(slot * TILE, TILE), TILE)

    def row_copy(o, t, g, seq, head):
        return send(
            (keys, values)[t].at[:, pl.ds(g * D, D)], kv.at[t, z, slot_rows, :],
            a_send.at[o, t, g], a_recv.at[o, t, slot], seq, head,
        )

    for t in range(2):
        for o, plane in enumerate(near):
            for g, (seq, head, other) in enumerate(takers(plane)):
                pl.when(other)(row_copy(o, t, g, seq, head).start)

                @pl.when(jnp.logical_not(other))
                def _():
                    kv[t, z, slot_rows, :] = (keys, values)[t][:, g * D : (g + 1) * D]

    def rows_come(o, t):
        plane = (z, under[1], above[1])[o]
        for at, (seq, head, other) in enumerate(givers(plane)):
            landed = send(
                keys.at[:, pl.ds(0, D)], kv.at[t, plane, pl.ds(at * TILE, TILE), :],
                a_send.at[o, t, 0], a_recv.at[o, t, at], seq, head,
            )
            pl.when(other)(landed.wait_recv)

    def y_copy(k):
        src = (qt.at[0, mine], gt.at[0, mine], lay, st.at[0, c])[k]
        dst = (qt.at[1, mine], gt.at[1, mine], l_in, st.at[1, c])[k]
        return send(src, dst, y_send.at[k], y_recv.at[k], s, pair)

    d_copies = [
        send(qt.at[0, mine], qt.at[0, mine], d_send.at[0], d_recv.at[0], twin, h),
        send(gt.at[0, mine], gt.at[0, mine], d_send.at[1], d_recv.at[1], twin, h),
        send(st.at[0, c], st.at[0, c], d_send.at[2], d_recv.at[2], twin, h),
    ]
    for copy in (y_copy(0), d_copies[0], d_copies[1], y_copy(1)):
        copy.start()
    for load in loads[4:]:
        load.wait()

    ones = jnp.ones((8, D), BF16)
    for hh in range(2):
        lay[hh * NBLK : (hh + 1) * NBLK, :] = layout[hh].astype(F32).astype(BF16)
        for rb in range(4):
            at = (slice(rb * BLOCK, (rb + 1) * BLOCK), slice(hh * D, (hh + 1) * D))
            product = grads[at].astype(F32) * outs[at].astype(F32)
            high = product.astype(BF16)
            low = (product - high.astype(F32)).astype(BF16)
            total = dot(ones, high, NT) + dot(ones, low, NT)
            row = hh * 4 + rb
            st[0, c, row : row + 1, :] = norms[hh : hh + 1, rb * BLOCK : (rb + 1) * BLOCK]
            st[0, c, 8 + row : 9 + row, :] = total[0:1, :]
    for copy in (y_copy(3), d_copies[2], y_copy(2)):
        copy.start()
    acc[...] = jnp.zeros_like(acc)
    dqt[...] = jnp.zeros_like(dqt)
    qx[...] = jnp.zeros_like(qx)
    gx[...] = jnp.zeros_like(gx)
    pick[...] = jnp.zeros_like(pick)

    lane = iota((1, D), 1)
    placed = jnp.zeros((1, D), jnp.int32)
    for sb in range(NBLK):
        placed = jnp.where(lane == sb, order[sb], placed)
    order_v[...] = placed
    first, after = jnp.zeros((1, D), F32), jnp.full((1, D), float(ALWAYS), F32)
    row8 = iota((8, COLS), 0)
    first_row, after_row = jnp.zeros((8, COLS), F32), jnp.full((8, COLS), float(ALWAYS), F32)
    for d in range(1, 8):
        below = jnp.sum((ids[...] < d).astype(F32), axis=(0, 1), keepdims=True)
        first = jnp.where(lane == AT_DOC + d, below, first)
        after = jnp.where(lane == AT_DOC + d - 1, below, after)
        first_row = jnp.where(row8 == d, below, first_row)
        after_row = jnp.where(row8 == d - 1, below, after_row)
    spans[0:1, :] = first.astype(jnp.int32)
    spans[1:2, :] = after.astype(jnp.int32)
    docs[0] = first_row.astype(jnp.int32)
    docs[1] = after_row.astype(jnp.int32)

    stored = (iota((NBLK, D), 0) == order_v[...]) & (iota((NBLK, D), 1) < NBLK)
    stored = stored.astype(F32).astype(BF16)
    lperm[0] = dot(lay[...], stored, NN)
    ahead[...] = quarter * TILE + iota((TILE, COLS), 0) - iota((TILE, COLS), 1) % BLOCK
    spread = (iota((8, COLS), 1) // BLOCK == iota((8, COLS), 0)).astype(F32)
    doc_lane = (lane >= AT_DOC) & (lane < AT_ONE)

    def prepare(side, cb):
        for rp in range(2):
            unit = cb * 2 + rp
            norm, delta, position = [], [], []
            for b in range(2):
                block = order[z * 8 + unit * 2 + b]
                for hh in range(2):
                    at, row = b * 2 + hh, hh * 4 + rp * 2 + b
                    norm.append(st[side, cb, row : row + 1, :])
                    delta.append(st[side, cb, 8 + row : 9 + row, :])
                    position.append(block * BLOCK + iota((1, BLOCK), 1))
                    seen = lperm[side, pl.ds(hh * NBLK + block, 1), :]
                    pick[at : at + 1, :] = jnp.where((seen > 0.5) & (order_v[...] <= block), 1.0, 0.0)
            norm = three(jnp.concatenate(norm, axis=1) * (-1.0 / SCALE))
            delta = three(-jnp.concatenate(delta, axis=1))
            position = jnp.concatenate(position, axis=1)
            seen = dot(pick[...], spread, TN)
            qx[side, unit, 0:NBLK, :] = jnp.where(seen[0:NBLK, :] > 0.5, 0.0, -BIG).astype(BF16)
            inside = (position >= docs[0]) & (position < docs[1])
            zero = jnp.zeros((8, COLS), F32)
            for ref, rows, head in ((qx, norm, jnp.where(inside, 0.0, -BIG)), (gx, delta, zero)):
                parts = zero
                for i in range(3):
                    parts = jnp.where(row8 == i, rows[i].astype(F32), parts)
                ref[side, unit, AT_DOC : AT_DOC + 16, :] = jnp.concatenate([head, parts], axis=0).astype(BF16)

    def prepare_keys(plane):
        row, col = iota((TILE, D), 0), iota((TILE, D), 1)
        for t in range(TILES):
            position = order[plane * TILES + t] * BLOCK + quarter * TILE + row
            hot = col == plane * TILES + t
            hot = hot | (doc_lane & (position >= spans[0:1, :]) & (position < spans[1:2, :]))
            hot = hot | ((col >= AT_ONE) & (col < AT_ONE + 3))
            ax[plane, pl.ds(t * TILE, TILE), :] = hot.astype(F32).astype(BF16)

    def spot(n):
        side = n // 32
        j = n % 32 // 4
        j = j + side * (7 - 2 * j)
        unit = n % 4
        m = n - 52
        late = jnp.where(m >= 0, 1, 0)
        k = m // 3
        j = j + late * (2 - m % 3 - j)
        unit = unit + late * ((k // 2 * (2 * c - 1) + 1 - c) * 2 + k % 2 - unit)
        away = (j + 1) // 2
        return (z + NZ + away * (1 - 2 * (j % 2))) % NZ, side, unit

    def front(n):
        plane, side, unit = spot(n)
        extra = ax[plane]
        scores = dot(
            jnp.concatenate([kv[0, plane], extra], 1), jnp.concatenate([qt[side, unit], qx[side, unit]], 0), NN
        )
        grads_less = dot(
            jnp.concatenate([kv[1, plane], extra], 1), jnp.concatenate([gt[side, unit], gx[side, unit]], 0), NN
        )
        low, score_grad = [], []
        for t in range(TILES):
            part = slice(t * TILE, (t + 1) * TILE)
            bound = []
            for b in range(2):
                same = order[plane * TILES + t] == order[z * 8 + unit * 2 + b]
                bound.append(jnp.full((1, 2 * BLOCK), jnp.where(same, 0, ALWAYS), jnp.int32))
            visible = ahead[...] <= jnp.concatenate(bound, axis=1)
            weights = jnp.where(visible, jnp.exp2(scores[part, :] * (SCALE * LOG2E)), 0.0)
            low.append(weights.astype(BF16))
            score_grad.append((weights * grads_less[part, :]).astype(BF16))
        return jnp.concatenate(low, axis=0), jnp.concatenate(score_grad, axis=0)

    def back(n, low, score_grad):
        plane, side, unit = spot(n)
        acc[0, plane] += dot(qt[side, unit], score_grad, NT)
        acc[1, plane] += dot(gt[side, unit], low, NT)
        dqt[side, unit] += dot(kv[0, plane], score_grad, TN)

    def query_sums(side, cb, blocks=range(4)):
        for rb in blocks:
            for hh in range(2):
                at = (rb % 2 * 2 + hh) * BLOCK
                block_grad = dqt[side, cb * 2 + rb // 2, :, at : at + BLOCK].T * SCALE
                dqp[side, cb, rb * BLOCK : (rb + 1) * BLOCK, hh * D : (hh + 1) * D] = block_grad

    def key_copy(way, step, t):
        piece = kv.at[t, under[step - 1] if way == 0 else above[step - 1]]
        return send(
            piece, piece, k_send.at[way, step - 1, t], k_recv.at[way, step - 1, t],
            up if way == 0 else down, h,
        )

    def carries(way, step, t):
        return step < 4 or (step == 4 and t == way)

    def arrive(step, t):
        for way in range(2):
            if carries(way, step, t):
                key_copy(way, step, t).wait_recv()
            if carries(way, step + 1, t):
                key_copy(way, step + 1, t).start()

    def forward(k):
        src = (qt.at[1, mine], gt.at[1, mine], None, st.at[1, c])[k]
        return send(src, src, f_send.at[k], f_recv.at[k], twin, h)

    def pass_on(k):
        y_copy(k).wait_recv()
        forward(k).start()

    def sum_copy(way, step, t):
        return send(
            z_out.at[way, step - 1, t], z_in.at[way, step - 1, t],
            z_send.at[way, step - 1, t], z_recv.at[way, step - 1, t],
            up if way == 0 else down, h,
        )

    def pass_sum(way, step, t):
        value = acc[t, (above if way == 0 else under)[5 - step]]
        if step > 2 or (step == 2 and t == way):
            sum_copy(way, step - 1, t).wait_recv()
            value = value + z_in[way, step - 2, t].astype(F32)
        z_out[way, step - 1, t] = value.astype(BF16)
        sum_copy(way, step, t).start()

    def twin_copy(side):
        return send(dqp.at[side, 1 - c], twin_in.at[side], r_send.at[side], r_recv.at[side], twin, h)

    def twin_sums(side):
        query_sums(side, 1 - c)
        twin_copy(side).start()

    def pair_copy(rp):
        rows = pl.ds(rp * 2 * BLOCK, 2 * BLOCK)
        return send(
            pair_out.at[rows, :], pair_in.at[rows, :], r_send.at[2 + rp], r_recv.at[2 + rp], s, pair
        )

    def pair_sums(rp):
        query_sums(1, c, range(rp * 2, rp * 2 + 2))
        if rp == 0:
            twin_copy(1).wait_recv()
        rows = slice(rp * 2 * BLOCK, (rp + 1) * 2 * BLOCK)
        pair_out[rows, :] = (dqp[1, c, rows, :] + twin_in[1, rows, :]).astype(BF16)
        pair_copy(rp).start()

    mine_g = x * 2 + y // 2

    def way_copy(way, t, k, seq, head):
        return send(
            fin_way.at[way, k, t], way_in.at[way, mine_g, t],
            w_send.at[way, t, k], w_recv.at[way, t, mine_g], seq, head,
        )

    def last_sum(way, t):
        plane = (above if way == 0 else under)[1]
        sum_copy(way, 3, t).wait_recv()
        value = (acc[t, plane] + z_in[way, 2, t].astype(F32)).T.astype(BF16)
        for k, (seq, head, _) in enumerate(givers(plane)):
            fin_way[way, k, t] = value[k * TILE : (k + 1) * TILE, :]
        for k, (seq, head, _) in enumerate(givers(plane)):
            way_copy(way, t, k, seq, head).start()

    prepare(0, c)
    for plane in near:
        prepare_keys(plane)
    for copy in d_copies:
        copy.wait_recv()
    prepare(0, 1 - c)
    for t in range(2):
        rows_come(0, t)
        for way in range(2):
            rows_come(1 + way, t)
            key_copy(way, 2, t).start()
    lows[0], sgs[0] = front(z * 0)

    def planes_at(away):
        prepare_keys(under[away])
        if away < 4:
            prepare_keys(above[away])

    def heads_come():
        pass_on(1)
        pass_on(3)
        y_copy(2).wait_recv()

    def other_heads():
        lperm[1] = dot(l_in[...], stored, NN)
        prepare(1, c)
        for k in (0, 1, 3):
            forward(k).wait_recv()
        prepare(1, 1 - c)

    def sums(*which):
        for w in which:
            pass_sum(*w)

    events = {
        4: lambda: (planes_at(2), arrive(2, 0)),
        5: lambda: arrive(2, 1),
        6: lambda: pass_on(0),
        8: lambda: (planes_at(3), arrive(3, 0)),
        9: lambda: arrive(3, 1),
        11: lambda: (planes_at(4), arrive(4, 0)),
        13: lambda: (heads_come(), arrive(4, 1)),
        15: lambda: other_heads(),
        18: lambda: sums((0, 1, 0), (1, 1, 1)),
        20: lambda: sums((0, 2, 1)),
        21: lambda: twin_sums(0),
        22: lambda: sums((0, 2, 0), (1, 2, 0), (1, 2, 1)),
        24: lambda: sums((0, 3, 1)),
        26: lambda: sums((0, 3, 0), (1, 3, 0)),
        28: lambda: sums((1, 3, 1)),
        29: lambda: twin_sums(1),
        31: lambda: (last_sum(0, 1), last_sum(0, 0), pair_sums(0)),
    }

    def two(i, _):
        for at, event in events.items():
            pl.when(i == at)(lambda event=event: (event(), None)[1])
        n = 2 * i
        lows[1], sgs[1] = front(n + 1)
        back(n, lows[0], sgs[0])
        lows[0], sgs[0] = front(jnp.minimum(n + 2, 63))
        back(n + 1, lows[1], sgs[1])
        return 0

    lax.fori_loop(0, 32, two, 0)

    last_sum(1, 0)
    last_sum(1, 1)
    pair_sums(1)

    def own_copy(k, seq, head):
        return send(fin.at[k], own_in.at[mine_g], b_send.at[k], b_recv.at[mine_g], seq, head)

    for t in range(2):
        value = acc[t, z].T
        for k in range(8):
            fin[k, t] = value[k * TILE : (k + 1) * TILE, :]
    for k, (seq, head, other) in enumerate(givers(z)):
        pl.when(other)(own_copy(k, seq, head).start)

        @pl.when(jnp.logical_not(other))
        def _():
            own_in[mine_g] = fin[k]

    query_sums(0, c)
    twin_copy(0).wait_recv()
    dq[...] = dqp[0, c] + twin_in[0]

    for way in range(2):
        for t in range(2):
            for g, (seq, head, _) in enumerate(takers((under if way == 0 else above)[1])):
                send(
                    fin_way.at[way, 0, t], way_in.at[way, g, t],
                    w_send.at[way, t, 0], w_recv.at[way, t, g], seq, head,
                ).wait_recv()
    for g, (seq, head, other) in enumerate(takers(z)):
        landed = send(fin.at[0], own_in.at[g], b_send.at[0], b_recv.at[g], seq, head)
        pl.when(other)(landed.wait_recv)
    for rp in range(2):
        pair_copy(rp).wait_recv()

    for o, plane in enumerate(near):
        for g, (seq, head, other) in enumerate(takers(plane)):
            for t in range(2):
                pl.when(other)(row_copy(o, t, g, seq, head).wait_send)
    for k, (seq, head, other) in enumerate(givers(z)):
        pl.when(other)(own_copy(k, seq, head).wait_send)
    for way in range(2):
        for t in range(2):
            for step in range(2, 5):
                if carries(way, step, t):
                    key_copy(way, step, t).wait_send()
            for step in range(1, 4):
                if step > 1 or t == way:
                    sum_copy(way, step, t).wait_send()
            for k, (seq, head, _) in enumerate(givers((above if way == 0 else under)[1])):
                way_copy(way, t, k, seq, head).wait_send()
    for k in range(4):
        y_copy(k).wait_send()
        if k != 2:
            forward(k).wait_send()
    for copy in d_copies + [twin_copy(0), twin_copy(1), pair_copy(0), pair_copy(1)]:
        copy.wait_send()


def fused(keys, values, queries, grads, outs, norms, layout, ids, order):
    vmem = pl.BlockSpec(memory_space=pltpu.VMEM)
    hbm = pl.BlockSpec(memory_space=pltpu.HBM)
    dma = pltpu.SemaphoreType.DMA
    v = pltpu.VMEM
    return pl.pallas_call(
        fused_kernel,
        name="fused",
        out_shape=(
            jax.ShapeDtypeStruct((ROWS, 2 * D), F32),
            jax.ShapeDtypeStruct((ROWS, 2 * D), BF16),
            jax.ShapeDtypeStruct((8, 2, TILE, D), F32),
            jax.ShapeDtypeStruct((2, 8, 2, TILE, D), BF16),
        ),
        in_specs=[hbm] * 9,
        out_specs=(vmem,) * 4,
        scratch_shapes=[
            v((TILE, 8 * D), BF16), v((TILE, 8 * D), BF16),
            v((ROWS, 2 * D), BF16), v((ROWS, 2 * D), BF16), v((ROWS, 2 * D), BF16),
            v((2, ROWS), F32), v((2, NBLK, NBLK), jnp.int32),
            v((NBLK, BLOCK), jnp.int32), pltpu.SMEM((NBLK,), jnp.int32), v((1, D), jnp.int32),
            v((2, NZ, PLANE, D), BF16),
            v((2, 4, D, COLS), BF16), v((2, 4, D, COLS), BF16),
            v((2, 2, 16, BLOCK), F32),
            v((2 * NBLK, NBLK), BF16), v((2 * NBLK, NBLK), BF16),
            v((2, 2 * NBLK, D), F32), v((8, D), jnp.int32), v((2, 8, COLS), jnp.int32),
            v((NZ, PLANE, D), BF16),
            v((2, 4, D, COLS), BF16), v((2, 4, D, COLS), BF16),
            v((2, PLANE, COLS), BF16), v((2, PLANE, COLS), BF16),
            v((2, NZ, D, PLANE), F32),
            v((2, 4, D, COLS), F32),
            v((2, 2, ROWS, 2 * D), F32),
            v((2, ROWS, 2 * D), F32), v((ROWS, 2 * D), BF16),
            v((2, 4, 2, D, PLANE), BF16), v((2, 4, 2, D, PLANE), BF16),
            v((8, 2, TILE, D), F32), v((2, 8, 2, TILE, D), BF16),
            v((TILE, COLS), jnp.int32), v((8, D), F32),
            dma((9,)), dma((3, 2, 8)), dma((3, 2, 8)),
            dma((2, 4, 2)), dma((2, 4, 2)), dma((2, 4, 2)), dma((2, 4, 2)),
            dma((4,)), dma((4,)), dma((3,)), dma((3,)),
            dma((4,)), dma((4,)), dma((4,)), dma((4,)), dma((8,)), dma((8,)), dma((2, 2, 8)), dma((2, 2, 8)),
        ],
        compiler_params=pltpu.CompilerParams(
            collective_id=0, has_side_effects=True, vmem_limit_bytes=60 * MIB
        ),
    )(keys, values, queries, grads, outs, norms, layout, ids, order)


def finish_kernel(sums, pair_in, own_in, way_in, dq, dk, dv):
    dq[...] = sums[...] + pair_in[...].astype(F32)
    for g in range(8):
        for t, (ref, scale) in enumerate(((dk, SCALE), (dv, 1.0))):
            total = own_in[g, t] + way_in[0, g, t].astype(F32) + way_in[1, g, t].astype(F32)
            ref[:, g * D : (g + 1) * D] = total * scale


def finish(sums, pair_in, own_in, way_in):
    vmem = pl.BlockSpec(memory_space=pltpu.VMEM)
    return pl.pallas_call(
        finish_kernel,
        name="finish",
        out_shape=(
            jax.ShapeDtypeStruct((ROWS, 2 * D), F32),
            jax.ShapeDtypeStruct((TILE, 8 * D), F32),
            jax.ShapeDtypeStruct((TILE, 8 * D), F32),
        ),
        in_specs=[vmem] * 4,
        out_specs=(vmem,) * 3,
        compiler_params=pltpu.CompilerParams(vmem_limit_bytes=60 * MIB),
    )(sums, pair_in, own_in, way_in)


def body(
    queries, keys, values, attn_out, out_grad, log_norm, block_layout, document_ids, block_order
):
    return finish(
        *fused(
            keys,
            values,
            queries,
            out_grad,
            attn_out,
            log_norm,
            block_layout,
            document_ids.reshape(NBLK, BLOCK),
            block_order,
        )
    )


def solution(mesh):
    in_specs = (
        P("seq", "head"),
        P(("seq", "head"), None),
        P(("seq", "head"), None),
        P("seq", "head"),
        P("seq", "head"),
        P("head", "seq"),
        P("head", None, None),
        P(),
        P(),
    )
    out_specs = (P("seq", "head"), P(("seq", "head"), None), P(("seq", "head"), None))
    return jax.shard_map(body, mesh=mesh, in_specs=in_specs, out_specs=out_specs, check_vma=False)
```

```python
import jax
import jax.numpy as jnp
from jax import lax
from jax.experimental import pallas as pl
from jax.experimental.pallas import tpu as pltpu
from jax.sharding import PartitionSpec as P

MESH = pl.DeviceIdType.MESH
D = 128
BLOCK = 128
NBLK = 64
NZ = 8
TILE = 32
TILES = 8
PLANE = TILE * TILES
ROWS = 512
COLS = 512
BIG = 1e30
ALWAYS = 1 << 20
SCALE = D ** (-0.5)
LOG2E = 1.4426950408889634
BF16 = jnp.bfloat16
F32 = jnp.float32
NN = (((1,), (0,)), ((), ()))
NT = (((1,), (1,)), ((), ()))
TN = (((0,), (0,)), ((), ()))
AT_DOC = 64
AT_ONE = 72
MIB = 1 << 20


def place():
    s = lax.axis_index("seq")
    h = lax.axis_index("head")
    return s, h, s // 2, s % 2, h // 4, h % 4


def send(src, dst, send_sem, recv_sem, seq, head):
    return pltpu.make_async_remote_copy(
        src_ref=src,
        dst_ref=dst,
        send_sem=send_sem,
        recv_sem=recv_sem,
        device_id=(seq, head),
        device_id_type=MESH,
    )


def dot(a, b, dims):
    return lax.dot_general(a, b, dims, preferred_element_type=F32)


def three(x):
    high = x.astype(BF16)
    rest = x - high.astype(F32)
    mid = rest.astype(BF16)
    low = (rest - mid.astype(F32)).astype(BF16)
    return [high, mid, low]


def iota(shape, dim):
    return lax.broadcasted_iota(jnp.int32, shape, dim)


def fused_kernel(
    keys_h, values_h, queries_h, grads_h, outs_h, norms_h, layout_h, ids_h, order_h,
    dq, pair_in, way_in,
    keys, values, queries, grads, outs, norms, layout, ids, order, order_v,
    kv, qt, gt, st, lay, l_in, lperm, spans, docs,
    ax, qx, gx, lows, sgs, acc, dqt, dqp, twin_in, pair_out, z_out, z_in, fin, ahead, pick,
    l_sem, a_send, a_recv, k_send, k_recv, z_send, z_recv, y_send, y_recv, d_send, d_recv,
    f_send, f_recv, r_send, r_recv, w_send, w_recv,
):
    s, h, z, c, x, y = place()
    pair = h + 1 - 2 * (y % 2)
    twin = s + 1 - 2 * c
    up = ((z + 1) % NZ) * 2 + c
    down = ((z + NZ - 1) % NZ) * 2 + c
    hp = y % 2
    inner = (y + 1) // 2 % 2
    quarter = inner + c * (3 - 2 * inner)

    loads = []
    for i, (src, dst) in enumerate((
        (queries_h, queries), (keys_h, keys), (values_h, values), (grads_h, grads), (outs_h, outs),
        (norms_h, norms), (layout_h, layout), (ids_h, ids), (order_h, order),
    )):
        loads.append(pltpu.make_async_copy(src, dst, l_sem.at[i]))
        loads[i].start()

    above = [(z + d) % NZ for d in range(5)]
    under = [(z + NZ - d) % NZ for d in range(5)]
    own = (y // 2 == c).astype(jnp.int32)

    def takers(plane):
        out = []
        for xg in range(4):
            for yp in range(2):
                head = xg * 4 + (inner if yp == 0 else 3 - inner)
                out.append((plane * 2 + y // 2, head, (plane * 2 + y // 2 != s) | (head != h)))
        return out

    def givers(plane):
        out = []
        for cg in range(2):
            for xg in range(4):
                seq, head = plane * 2 + cg, xg * 4 + quarter
                out.append((seq, head, (seq != s) | (head != h)))
        return out

    near = (z, above[1], under[1])
    barrier = pltpu.get_barrier_semaphore()
    for seq, head in ((s, pair), (twin, h), (up, h), (down, h)):
        pl.semaphore_signal(barrier, inc=1, device_id=(seq, head), device_id_type=MESH)
    for plane in near:
        for seq, head, other in takers(plane) + givers(plane):

            @pl.when(other)
            def _():
                pl.semaphore_signal(barrier, inc=1, device_id=(seq, head), device_id_type=MESH)

    mine = pl.ds(c * 2, 2)

    def columns(source, target):
        for rb in range(4):
            for hh in range(2):
                at = (rb % 2 * 2 + hh) * BLOCK
                block = source[rb * BLOCK : (rb + 1) * BLOCK, hh * D : (hh + 1) * D]
                target[0, c * 2 + rb // 2, :, at : at + BLOCK] = block.T

    loads[0].wait()
    columns(queries, qt)
    for load in loads[1:4]:
        load.wait()
    columns(grads, gt)
    pl.semaphore_wait(barrier, 4 + 48 - 2 * own)

    slot = c * 4 + x
    slot_rows = pl.ds(pl.multiple_of(slot * TILE, TILE), TILE)

    def row_copy(o, t, g, seq, head):
        return send(
            (keys, values)[t].at[:, pl.ds(g * D, D)], kv.at[t, z, slot_rows, :],
            a_send.at[o, t, g], a_recv.at[o, t, slot], seq, head,
        )

    for t in range(2):
        for o, plane in enumerate(near):
            for g, (seq, head, other) in enumerate(takers(plane)):
                pl.when(other)(row_copy(o, t, g, seq, head).start)

                @pl.when(jnp.logical_not(other))
                def _():
                    kv[t, z, slot_rows, :] = (keys, values)[t][:, g * D : (g + 1) * D]

    def rows_come(o, t):
        plane = (z, under[1], above[1])[o]
        for at, (seq, head, other) in enumerate(givers(plane)):
            landed = send(
                keys.at[:, pl.ds(0, D)], kv.at[t, plane, pl.ds(at * TILE, TILE), :],
                a_send.at[o, t, 0], a_recv.at[o, t, at], seq, head,
            )
            pl.when(other)(landed.wait_recv)

    def y_copy(k):
        src = (qt.at[0, mine], gt.at[0, mine], lay, st.at[0, c])[k]
        dst = (qt.at[1, mine], gt.at[1, mine], l_in, st.at[1, c])[k]
        return send(src, dst, y_send.at[k], y_recv.at[k], s, pair)

    d_copies = [
        send(qt.at[0, mine], qt.at[0, mine], d_send.at[0], d_recv.at[0], twin, h),
        send(gt.at[0, mine], gt.at[0, mine], d_send.at[1], d_recv.at[1], twin, h),
        send(st.at[0, c], st.at[0, c], d_send.at[2], d_recv.at[2], twin, h),
    ]
    for copy in (y_copy(0), d_copies[0], d_copies[1], y_copy(1)):
        copy.start()
    for load in loads[4:]:
        load.wait()

    ones = jnp.ones((8, D), BF16)
    for hh in range(2):
        lay[hh * NBLK : (hh + 1) * NBLK, :] = layout[hh].astype(F32).astype(BF16)
        for rb in range(4):
            at = (slice(rb * BLOCK, (rb + 1) * BLOCK), slice(hh * D, (hh + 1) * D))
            product = grads[at].astype(F32) * outs[at].astype(F32)
            high = product.astype(BF16)
            low = (product - high.astype(F32)).astype(BF16)
            total = dot(ones, high, NT) + dot(ones, low, NT)
            row = hh * 4 + rb
            st[0, c, row : row + 1, :] = norms[hh : hh + 1, rb * BLOCK : (rb + 1) * BLOCK]
            st[0, c, 8 + row : 9 + row, :] = total[0:1, :]
    for copy in (y_copy(3), d_copies[2], y_copy(2)):
        copy.start()
    acc[...] = jnp.zeros_like(acc)
    dqt[...] = jnp.zeros_like(dqt)
    qx[...] = jnp.zeros_like(qx)
    gx[...] = jnp.zeros_like(gx)
    pick[...] = jnp.zeros_like(pick)

    lane = iota((1, D), 1)
    placed = jnp.zeros((1, D), jnp.int32)
    for sb in range(NBLK):
        placed = jnp.where(lane == sb, order[sb], placed)
    order_v[...] = placed
    first, after = jnp.zeros((1, D), F32), jnp.full((1, D), float(ALWAYS), F32)
    row8 = iota((8, COLS), 0)
    first_row, after_row = jnp.zeros((8, COLS), F32), jnp.full((8, COLS), float(ALWAYS), F32)
    for d in range(1, 8):
        below = jnp.sum((ids[...] < d).astype(F32), axis=(0, 1), keepdims=True)
        first = jnp.where(lane == AT_DOC + d, below, first)
        after = jnp.where(lane == AT_DOC + d - 1, below, after)
        first_row = jnp.where(row8 == d, below, first_row)
        after_row = jnp.where(row8 == d - 1, below, after_row)
    spans[0:1, :] = first.astype(jnp.int32)
    spans[1:2, :] = after.astype(jnp.int32)
    docs[0] = first_row.astype(jnp.int32)
    docs[1] = after_row.astype(jnp.int32)

    stored = (iota((NBLK, D), 0) == order_v[...]) & (iota((NBLK, D), 1) < NBLK)
    stored = stored.astype(F32).astype(BF16)
    lperm[0] = dot(lay[...], stored, NN)
    ahead[...] = quarter * TILE + iota((TILE, COLS), 0) - iota((TILE, COLS), 1) % BLOCK
    spread = (iota((8, COLS), 1) // BLOCK == iota((8, COLS), 0)).astype(F32)
    doc_lane = (lane >= AT_DOC) & (lane < AT_ONE)

    def prepare(side, cb):
        for rp in range(2):
            unit = cb * 2 + rp
            norm, delta, position = [], [], []
            for b in range(2):
                block = order[z * 8 + unit * 2 + b]
                for hh in range(2):
                    at, row = b * 2 + hh, hh * 4 + rp * 2 + b
                    norm.append(st[side, cb, row : row + 1, :])
                    delta.append(st[side, cb, 8 + row : 9 + row, :])
                    position.append(block * BLOCK + iota((1, BLOCK), 1))
                    seen = lperm[side, pl.ds(hh * NBLK + block, 1), :]
                    pick[at : at + 1, :] = jnp.where((seen > 0.5) & (order_v[...] <= block), 1.0, 0.0)
            norm = three(jnp.concatenate(norm, axis=1) * (-1.0 / SCALE))
            delta = three(-jnp.concatenate(delta, axis=1))
            position = jnp.concatenate(position, axis=1)
            seen = dot(pick[...], spread, TN)
            qx[side, unit, 0:NBLK, :] = jnp.where(seen[0:NBLK, :] > 0.5, 0.0, -BIG).astype(BF16)
            inside = (position >= docs[0]) & (position < docs[1])
            zero = jnp.zeros((8, COLS), F32)
            for ref, rows, head in ((qx, norm, jnp.where(inside, 0.0, -BIG)), (gx, delta, zero)):
                parts = zero
                for i in range(3):
                    parts = jnp.where(row8 == i, rows[i].astype(F32), parts)
                ref[side, unit, AT_DOC : AT_DOC + 16, :] = jnp.concatenate([head, parts], axis=0).astype(BF16)

    def prepare_keys(plane):
        row, col = iota((TILE, D), 0), iota((TILE, D), 1)
        for t in range(TILES):
            position = order[plane * TILES + t] * BLOCK + quarter * TILE + row
            hot = col == plane * TILES + t
            hot = hot | (doc_lane & (position >= spans[0:1, :]) & (position < spans[1:2, :]))
            hot = hot | ((col >= AT_ONE) & (col < AT_ONE + 3))
            ax[plane, pl.ds(t * TILE, TILE), :] = hot.astype(F32).astype(BF16)

    def spot(n):
        side = n // 32
        j = n % 32 // 4
        j = j + side * (7 - 2 * j)
        unit = n % 4
        m = n - 52
        late = jnp.where(m >= 0, 1, 0)
        k = m // 3
        j = j + late * (2 - m % 3 - j)
        unit = unit + late * ((k // 2 * (2 * c - 1) + 1 - c) * 2 + k % 2 - unit)
        away = (j + 1) // 2
        return (z + NZ + away * (1 - 2 * (j % 2))) % NZ, side, unit

    def front(n):
        plane, side, unit = spot(n)
        extra = ax[plane]
        scores = dot(
            jnp.concatenate([kv[0, plane], extra], 1), jnp.concatenate([qt[side, unit], qx[side, unit]], 0), NN
        )
        grads_less = dot(
            jnp.concatenate([kv[1, plane], extra], 1), jnp.concatenate([gt[side, unit], gx[side, unit]], 0), NN
        )
        low, score_grad = [], []
        for t in range(TILES):
            part = slice(t * TILE, (t + 1) * TILE)
            bound = []
            for b in range(2):
                same = order[plane * TILES + t] == order[z * 8 + unit * 2 + b]
                bound.append(jnp.full((1, 2 * BLOCK), jnp.where(same, 0, ALWAYS), jnp.int32))
            visible = ahead[...] <= jnp.concatenate(bound, axis=1)
            weights = jnp.where(visible, jnp.exp2(scores[part, :] * (SCALE * LOG2E)), 0.0)
            low.append(weights.astype(BF16))
            score_grad.append((weights * grads_less[part, :]).astype(BF16))
        return jnp.concatenate(low, axis=0), jnp.concatenate(score_grad, axis=0)

    def back(n, low, score_grad):
        plane, side, unit = spot(n)
        acc[0, plane] += dot(qt[side, unit], score_grad, NT)
        acc[1, plane] += dot(gt[side, unit], low, NT)
        dqt[side, unit] += dot(kv[0, plane], score_grad, TN)

    def query_sums(side, cb, blocks=range(4)):
        for rb in blocks:
            for hh in range(2):
                at = (rb % 2 * 2 + hh) * BLOCK
                block_grad = dqt[side, cb * 2 + rb // 2, :, at : at + BLOCK].T * SCALE
                dqp[side, cb, rb * BLOCK : (rb + 1) * BLOCK, hh * D : (hh + 1) * D] = block_grad

    def key_copy(way, step, t):
        piece = kv.at[t, under[step - 1] if way == 0 else above[step - 1]]
        return send(
            piece, piece, k_send.at[way, step - 1, t], k_recv.at[way, step - 1, t],
            up if way == 0 else down, h,
        )

    def carries(way, step, t):
        return step < 4 or (step == 4 and t == way)

    def arrive(step, t):
        for way in range(2):
            if carries(way, step, t):
                key_copy(way, step, t).wait_recv()
            if carries(way, step + 1, t):
                key_copy(way, step + 1, t).start()

    def forward(k):
        src = (qt.at[1, mine], gt.at[1, mine], None, st.at[1, c])[k]
        return send(src, src, f_send.at[k], f_recv.at[k], twin, h)

    def pass_on(k):
        y_copy(k).wait_recv()
        forward(k).start()

    def sum_copy(way, step, t):
        return send(
            z_out.at[way, step - 1, t], z_in.at[way, step - 1, t],
            z_send.at[way, step - 1, t], z_recv.at[way, step - 1, t],
            up if way == 0 else down, h,
        )

    def pass_sum(way, step, t):
        value = acc[t, (above if way == 0 else under)[5 - step]]
        if step > 2 or (step == 2 and t == way):
            sum_copy(way, step - 1, t).wait_recv()
            value = value + z_in[way, step - 2, t].astype(F32)
        z_out[way, step - 1, t] = value.astype(BF16)
        sum_copy(way, step, t).start()

    def twin_copy(side):
        return send(dqp.at[side, 1 - c], twin_in.at[side], r_send.at[side], r_recv.at[side], twin, h)

    def twin_sums(side):
        query_sums(side, 1 - c)
        twin_copy(side).start()

    def pair_copy(rp):
        rows = pl.ds(rp * 2 * BLOCK, 2 * BLOCK)
        return send(
            pair_out.at[rows, :], pair_in.at[rows, :], r_send.at[2 + rp], r_recv.at[2 + rp], s, pair
        )

    def pair_sums(rp):
        query_sums(1, c, range(rp * 2, rp * 2 + 2))
        if rp == 0:
            twin_copy(1).wait_recv()
        rows = slice(rp * 2 * BLOCK, (rp + 1) * 2 * BLOCK)
        pair_out[rows, :] = (dqp[1, c, rows, :] + twin_in[1, rows, :]).astype(BF16)
        pair_copy(rp).start()

    mine_g = x * 2 + y // 2

    def way_copy(way, t, k, seq, head):
        return send(
            fin.at[way, k, t], way_in.at[way, mine_g, t],
            w_send.at[way, t, k], w_recv.at[way, t, mine_g], seq, head,
        )

    def last_sum(way, t):
        plane = (above if way == 0 else under)[1]
        sum_copy(way, 3, t).wait_recv()
        value = (acc[t, plane] + z_in[way, 2, t].astype(F32)).T.astype(BF16)
        for k, (seq, head, _) in enumerate(givers(plane)):
            fin[way, k, t] = value[k * TILE : (k + 1) * TILE, :]
        for k, (seq, head, _) in enumerate(givers(plane)):
            way_copy(way, t, k, seq, head).start()

    prepare(0, c)
    for plane in near:
        prepare_keys(plane)
    for copy in d_copies:
        copy.wait_recv()
    prepare(0, 1 - c)
    for t in range(2):
        rows_come(0, t)
        for way in range(2):
            rows_come(1 + way, t)
            key_copy(way, 2, t).start()
    lows[0], sgs[0] = front(z * 0)

    def planes_at(away):
        prepare_keys(under[away])
        if away < 4:
            prepare_keys(above[away])

    def heads_come():
        pass_on(1)
        pass_on(3)
        y_copy(2).wait_recv()

    def other_heads():
        lperm[1] = dot(l_in[...], stored, NN)
        prepare(1, c)
        for k in (0, 1, 3):
            forward(k).wait_recv()
        prepare(1, 1 - c)

    def sums(*which):
        for w in which:
            pass_sum(*w)

    events = {
        4: lambda: (planes_at(2), arrive(2, 0)),
        5: lambda: arrive(2, 1),
        6: lambda: pass_on(0),
        8: lambda: (planes_at(3), arrive(3, 0)),
        9: lambda: arrive(3, 1),
        11: lambda: (planes_at(4), arrive(4, 0)),
        13: lambda: (heads_come(), arrive(4, 1)),
        15: lambda: other_heads(),
        18: lambda: sums((0, 1, 0), (1, 1, 1)),
        20: lambda: sums((0, 2, 1)),
        21: lambda: twin_sums(0),
        22: lambda: sums((0, 2, 0), (1, 2, 0), (1, 2, 1)),
        24: lambda: sums((0, 3, 1)),
        26: lambda: sums((0, 3, 0), (1, 3, 0)),
        28: lambda: sums((1, 3, 1)),
        29: lambda: twin_sums(1),
        31: lambda: (last_sum(0, 1), last_sum(0, 0), pair_sums(0)),
    }

    def two(i, _):
        def happen(steps):
            if len(steps) == 1:
                pl.when(i == steps[0])(lambda: (events[steps[0]](), None)[1])
            else:
                mid = len(steps) // 2
                lax.cond(i < steps[mid], lambda: happen(steps[:mid]), lambda: happen(steps[mid:]))

        happen(sorted(events))
        n = 2 * i
        lows[1], sgs[1] = front(n + 1)
        back(n, lows[0], sgs[0])
        lows[0], sgs[0] = front(jnp.minimum(n + 2, 63))
        back(n + 1, lows[1], sgs[1])
        return 0

    lax.fori_loop(0, 32, two, 0)

    last_sum(1, 0)
    last_sum(1, 1)
    pair_sums(1)

    for t in range(2):
        value = acc[t, z].T.astype(BF16)
        for k in range(8):
            fin[2, k, t] = value[k * TILE : (k + 1) * TILE, :]
        for k, (seq, head, other) in enumerate(givers(z)):
            pl.when(other)(way_copy(2, t, k, seq, head).start)

            @pl.when(jnp.logical_not(other))
            def _():
                way_in[2, mine_g, t] = fin[2, k, t]

    query_sums(0, c)
    twin_copy(0).wait_recv()
    dq[...] = dqp[0, c] + twin_in[0]

    for way, plane in enumerate((under[1], above[1], z)):
        for t in range(2):
            for g, (seq, head, other) in enumerate(takers(plane)):
                landed = send(
                    fin.at[way, 0, t], way_in.at[way, g, t],
                    w_send.at[way, t, 0], w_recv.at[way, t, g], seq, head,
                )
                pl.when(other)(landed.wait_recv)
    for rp in range(2):
        pair_copy(rp).wait_recv()

    for o, plane in enumerate(near):
        for g, (seq, head, other) in enumerate(takers(plane)):
            for t in range(2):
                pl.when(other)(row_copy(o, t, g, seq, head).wait_send)
    for way, plane in enumerate((above[1], under[1], z)):
        for t in range(2):
            for k, (seq, head, other) in enumerate(givers(plane)):
                pl.when(other)(way_copy(way, t, k, seq, head).wait_send)
    for way in range(2):
        for t in range(2):
            for step in range(2, 5):
                if carries(way, step, t):
                    key_copy(way, step, t).wait_send()
            for step in range(1, 4):
                if step > 1 or t == way:
                    sum_copy(way, step, t).wait_send()
    for k in range(4):
        y_copy(k).wait_send()
        if k != 2:
            forward(k).wait_send()
    for copy in d_copies + [twin_copy(0), twin_copy(1), pair_copy(0), pair_copy(1)]:
        copy.wait_send()


def fused(keys, values, queries, grads, outs, norms, layout, ids, order):
    vmem = pl.BlockSpec(memory_space=pltpu.VMEM)
    hbm = pl.BlockSpec(memory_space=pltpu.HBM)
    dma = pltpu.SemaphoreType.DMA
    v = pltpu.VMEM
    return pl.pallas_call(
        fused_kernel,
        name="fused",
        out_shape=(
            jax.ShapeDtypeStruct((ROWS, 2 * D), F32),
            jax.ShapeDtypeStruct((ROWS, 2 * D), BF16),
            jax.ShapeDtypeStruct((3, 8, 2, TILE, D), BF16),
        ),
        in_specs=[hbm] * 9,
        out_specs=(vmem,) * 3,
        scratch_shapes=[
            v((TILE, 8 * D), BF16), v((TILE, 8 * D), BF16),
            v((ROWS, 2 * D), BF16), v((ROWS, 2 * D), BF16), v((ROWS, 2 * D), BF16),
            v((2, ROWS), F32), v((2, NBLK, NBLK), jnp.int32),
            v((NBLK, BLOCK), jnp.int32), pltpu.SMEM((NBLK,), jnp.int32), v((1, D), jnp.int32),
            v((2, NZ, PLANE, D), BF16),
            v((2, 4, D, COLS), BF16), v((2, 4, D, COLS), BF16),
            v((2, 2, 16, BLOCK), F32),
            v((2 * NBLK, NBLK), BF16), v((2 * NBLK, NBLK), BF16),
            v((2, 2 * NBLK, D), F32), v((8, D), jnp.int32), v((2, 8, COLS), jnp.int32),
            v((NZ, PLANE, D), BF16),
            v((2, 4, D, COLS), BF16), v((2, 4, D, COLS), BF16),
            v((2, PLANE, COLS), BF16), v((2, PLANE, COLS), BF16),
            v((2, NZ, D, PLANE), F32),
            v((2, 4, D, COLS), F32),
            v((2, 2, ROWS, 2 * D), F32),
            v((2, ROWS, 2 * D), F32), v((ROWS, 2 * D), BF16),
            v((2, 4, 2, D, PLANE), BF16), v((2, 4, 2, D, PLANE), BF16),
            v((3, 8, 2, TILE, D), BF16),
            v((TILE, COLS), jnp.int32), v((8, D), F32),
            dma((9,)), dma((3, 2, 8)), dma((3, 2, 8)),
            dma((2, 4, 2)), dma((2, 4, 2)), dma((2, 4, 2)), dma((2, 4, 2)),
            dma((4,)), dma((4,)), dma((3,)), dma((3,)),
            dma((4,)), dma((4,)), dma((4,)), dma((4,)), dma((3, 2, 8)), dma((3, 2, 8)),
        ],
        compiler_params=pltpu.CompilerParams(
            collective_id=0, has_side_effects=True, vmem_limit_bytes=60 * MIB
        ),
    )(keys, values, queries, grads, outs, norms, layout, ids, order)


def finish_kernel(sums, pair_in, way_in, dq, dk, dv):
    dq[...] = sums[...] + pair_in[...].astype(F32)
    for g in range(8):
        for t, (ref, scale) in enumerate(((dk, SCALE), (dv, 1.0))):
            total = way_in[2, g, t].astype(F32) + way_in[0, g, t].astype(F32) + way_in[1, g, t].astype(F32)
            ref[:, g * D : (g + 1) * D] = total * scale


def finish(sums, pair_in, way_in):
    vmem = pl.BlockSpec(memory_space=pltpu.VMEM)
    return pl.pallas_call(
        finish_kernel,
        name="finish",
        out_shape=(
            jax.ShapeDtypeStruct((ROWS, 2 * D), F32),
            jax.ShapeDtypeStruct((TILE, 8 * D), F32),
            jax.ShapeDtypeStruct((TILE, 8 * D), F32),
        ),
        in_specs=[vmem] * 3,
        out_specs=(vmem,) * 3,
        compiler_params=pltpu.CompilerParams(vmem_limit_bytes=60 * MIB),
    )(sums, pair_in, way_in)


def body(
    queries, keys, values, attn_out, out_grad, log_norm, block_layout, document_ids, block_order
):
    return finish(
        *fused(
            keys,
            values,
            queries,
            out_grad,
            attn_out,
            log_norm,
            block_layout,
            document_ids.reshape(NBLK, BLOCK),
            block_order,
        )
    )


def solution(mesh):
    in_specs = (
        P("seq", "head"),
        P(("seq", "head"), None),
        P(("seq", "head"), None),
        P("seq", "head"),
        P("seq", "head"),
        P("head", "seq"),
        P("head", None, None),
        P(),
        P(),
    )
    out_specs = (P("seq", "head"), P(("seq", "head"), None), P(("seq", "head"), None))
    return jax.shard_map(body, mesh=mesh, in_specs=in_specs, out_specs=out_specs, check_vma=False)
```

```python
import jax
import jax.numpy as jnp
from jax import lax
from jax.experimental import pallas as pl
from jax.experimental.pallas import tpu as pltpu
from jax.sharding import PartitionSpec as P

MESH = pl.DeviceIdType.MESH
D = 128
BLOCK = 128
NBLK = 64
NZ = 8
TILE = 32
TILES = 8
PLANE = TILE * TILES
ROWS = 512
COLS = 512
BIG = 1e30
ALWAYS = 1 << 20
SCALE = D ** (-0.5)
LOG2E = 1.4426950408889634
BF16 = jnp.bfloat16
F32 = jnp.float32
NN = (((1,), (0,)), ((), ()))
NT = (((1,), (1,)), ((), ()))
TN = (((0,), (0,)), ((), ()))
AT_DOC = 64
AT_ONE = 72
MIB = 1 << 20


def place():
    s = lax.axis_index("seq")
    h = lax.axis_index("head")
    return s, h, s // 2, s % 2, h // 4, h % 4


def send(src, dst, send_sem, recv_sem, seq, head):
    return pltpu.make_async_remote_copy(
        src_ref=src,
        dst_ref=dst,
        send_sem=send_sem,
        recv_sem=recv_sem,
        device_id=(seq, head),
        device_id_type=MESH,
    )


def dot(a, b, dims):
    return lax.dot_general(a, b, dims, preferred_element_type=F32)


def three(x):
    high = x.astype(BF16)
    rest = x - high.astype(F32)
    mid = rest.astype(BF16)
    low = (rest - mid.astype(F32)).astype(BF16)
    return [high, mid, low]


def iota(shape, dim):
    return lax.broadcasted_iota(jnp.int32, shape, dim)


def fused_kernel(
    keys_h, values_h, queries_h, grads_h, outs_h, norms_h, layout_h, ids_h, order_h,
    dq, pair_in, way_in,
    keys, values, queries, grads, outs, norms, layout, ids, order, order_v,
    kv, qt, gt, st, lay, l_in, lperm, spans, docs,
    ax, qx, gx, lows, sgs, acc, dqt, dqp, twin_in, pair_out, z_out, z_in, fin, ahead, pick,
    l_sem, a_send, a_recv, k_send, k_recv, z_send, z_recv, y_send, y_recv, d_send, d_recv,
    f_send, f_recv, r_send, r_recv, w_send, w_recv,
):
    s, h, z, c, x, y = place()
    pair = h + 1 - 2 * (y % 2)
    twin = s + 1 - 2 * c
    up = ((z + 1) % NZ) * 2 + c
    down = ((z + NZ - 1) % NZ) * 2 + c
    hp = y % 2
    inner = (y + 1) // 2 % 2
    quarter = inner + c * (3 - 2 * inner)

    loads = []
    for i, (src, dst) in enumerate((
        (queries_h, queries), (keys_h, keys), (values_h, values), (grads_h, grads), (outs_h, outs),
        (norms_h, norms), (layout_h, layout), (ids_h, ids), (order_h, order),
    )):
        loads.append(pltpu.make_async_copy(src, dst, l_sem.at[i]))
        loads[i].start()

    above = [(z + d) % NZ for d in range(5)]
    under = [(z + NZ - d) % NZ for d in range(5)]
    own = (y // 2 == c).astype(jnp.int32)

    def takers(plane):
        out = []
        for xg in range(4):
            for yp in range(2):
                head = xg * 4 + (inner if yp == 0 else 3 - inner)
                out.append((plane * 2 + y // 2, head, (plane * 2 + y // 2 != s) | (head != h)))
        return out

    def givers(plane):
        out = []
        for cg in range(2):
            for xg in range(4):
                seq, head = plane * 2 + cg, xg * 4 + quarter
                out.append((seq, head, (seq != s) | (head != h)))
        return out

    near = (z, above[1], under[1])
    barrier = pltpu.get_barrier_semaphore()
    for seq, head in ((s, pair), (twin, h), (up, h), (down, h)):
        pl.semaphore_signal(barrier, inc=1, device_id=(seq, head), device_id_type=MESH)
    for plane in near:
        for seq, head, other in givers(plane):

            @pl.when(other)
            def _():
                pl.semaphore_signal(barrier, inc=1, device_id=(seq, head), device_id_type=MESH)

    mine = pl.ds(c * 2, 2)

    def columns(source, target):
        for rb in range(4):
            for hh in range(2):
                at = (rb % 2 * 2 + hh) * BLOCK
                block = source[rb * BLOCK : (rb + 1) * BLOCK, hh * D : (hh + 1) * D]
                target[0, c * 2 + rb // 2, :, at : at + BLOCK] = block.T

    loads[0].wait()
    columns(queries, qt)
    for load in loads[1:4]:
        load.wait()
    columns(grads, gt)
    pl.semaphore_wait(barrier, 4 + 24 - own)

    slot = c * 4 + x
    slot_rows = pl.ds(pl.multiple_of(slot * TILE, TILE), TILE)

    def row_copy(o, t, g, seq, head):
        return send(
            (keys, values)[t].at[:, pl.ds(g * D, D)], kv.at[t, z, slot_rows, :],
            a_send.at[o, t, g], a_recv.at[o, t, slot], seq, head,
        )

    for t in range(2):
        for o, plane in enumerate(near):
            for g, (seq, head, other) in enumerate(takers(plane)):
                pl.when(other)(row_copy(o, t, g, seq, head).start)

                @pl.when(jnp.logical_not(other))
                def _():
                    kv[t, z, slot_rows, :] = (keys, values)[t][:, g * D : (g + 1) * D]

    def rows_come(o, t):
        plane = (z, under[1], above[1])[o]
        for at, (seq, head, other) in enumerate(givers(plane)):
            landed = send(
                keys.at[:, pl.ds(0, D)], kv.at[t, plane, pl.ds(at * TILE, TILE), :],
                a_send.at[o, t, 0], a_recv.at[o, t, at], seq, head,
            )
            pl.when(other)(landed.wait_recv)

    def y_copy(k):
        src = (qt.at[0, mine], gt.at[0, mine], lay, st.at[0, c])[k]
        dst = (qt.at[1, mine], gt.at[1, mine], l_in, st.at[1, c])[k]
        return send(src, dst, y_send.at[k], y_recv.at[k], s, pair)

    d_copies = [
        send(qt.at[0, mine], qt.at[0, mine], d_send.at[0], d_recv.at[0], twin, h),
        send(gt.at[0, mine], gt.at[0, mine], d_send.at[1], d_recv.at[1], twin, h),
        send(st.at[0, c], st.at[0, c], d_send.at[2], d_recv.at[2], twin, h),
    ]
    for copy in (y_copy(0), d_copies[0], d_copies[1], y_copy(1)):
        copy.start()
    for load in loads[4:]:
        load.wait()

    ones = jnp.ones((8, D), BF16)
    for hh in range(2):
        lay[hh * NBLK : (hh + 1) * NBLK, :] = layout[hh].astype(F32).astype(BF16)
        for rb in range(4):
            at = (slice(rb * BLOCK, (rb + 1) * BLOCK), slice(hh * D, (hh + 1) * D))
            product = grads[at].astype(F32) * outs[at].astype(F32)
            high = product.astype(BF16)
            low = (product - high.astype(F32)).astype(BF16)
            total = dot(ones, high, NT) + dot(ones, low, NT)
            row = hh * 4 + rb
            st[0, c, row : row + 1, :] = norms[hh : hh + 1, rb * BLOCK : (rb + 1) * BLOCK]
            st[0, c, 8 + row : 9 + row, :] = total[0:1, :]
    for copy in (y_copy(3), d_copies[2], y_copy(2)):
        copy.start()
    acc[...] = jnp.zeros_like(acc)
    dqt[...] = jnp.zeros_like(dqt)
    qx[...] = jnp.zeros_like(qx)
    gx[...] = jnp.zeros_like(gx)
    pick[...] = jnp.zeros_like(pick)

    lane = iota((1, D), 1)
    placed = jnp.zeros((1, D), jnp.int32)
    for sb in range(NBLK):
        placed = jnp.where(lane == sb, order[sb], placed)
    order_v[...] = placed
    first, after = jnp.zeros((1, D), F32), jnp.full((1, D), float(ALWAYS), F32)
    row8 = iota((8, COLS), 0)
    first_row, after_row = jnp.zeros((8, COLS), F32), jnp.full((8, COLS), float(ALWAYS), F32)
    for d in range(1, 8):
        below = jnp.sum((ids[...] < d).astype(F32), axis=(0, 1), keepdims=True)
        first = jnp.where(lane == AT_DOC + d, below, first)
        after = jnp.where(lane == AT_DOC + d - 1, below, after)
        first_row = jnp.where(row8 == d, below, first_row)
        after_row = jnp.where(row8 == d - 1, below, after_row)
    spans[0:1, :] = first.astype(jnp.int32)
    spans[1:2, :] = after.astype(jnp.int32)
    docs[0] = first_row.astype(jnp.int32)
    docs[1] = after_row.astype(jnp.int32)

    stored = (iota((NBLK, D), 0) == order_v[...]) & (iota((NBLK, D), 1) < NBLK)
    stored = stored.astype(F32).astype(BF16)
    lperm[0] = dot(lay[...], stored, NN)
    ahead[...] = quarter * TILE + iota((TILE, COLS), 0) - iota((TILE, COLS), 1) % BLOCK
    spread = (iota((8, COLS), 1) // BLOCK == iota((8, COLS), 0)).astype(F32)
    doc_lane = (lane >= AT_DOC) & (lane < AT_ONE)

    def prepare(side, cb):
        for rp in range(2):
            unit = cb * 2 + rp
            norm, delta, position = [], [], []
            for b in range(2):
                block = order[z * 8 + unit * 2 + b]
                for hh in range(2):
                    at, row = b * 2 + hh, hh * 4 + rp * 2 + b
                    norm.append(st[side, cb, row : row + 1, :])
                    delta.append(st[side, cb, 8 + row : 9 + row, :])
                    position.append(block * BLOCK + iota((1, BLOCK), 1))
                    seen = lperm[side, pl.ds(hh * NBLK + block, 1), :]
                    pick[at : at + 1, :] = jnp.where((seen > 0.5) & (order_v[...] <= block), 1.0, 0.0)
            norm = three(jnp.concatenate(norm, axis=1) * (-1.0 / SCALE))
            delta = three(-jnp.concatenate(delta, axis=1))
            position = jnp.concatenate(position, axis=1)
            seen = dot(pick[...], spread, TN)
            qx[side, unit, 0:NBLK, :] = jnp.where(seen[0:NBLK, :] > 0.5, 0.0, -BIG).astype(BF16)
            inside = (position >= docs[0]) & (position < docs[1])
            zero = jnp.zeros((8, COLS), F32)
            for ref, rows, head in ((qx, norm, jnp.where(inside, 0.0, -BIG)), (gx, delta, zero)):
                parts = zero
                for i in range(3):
                    parts = jnp.where(row8 == i, rows[i].astype(F32), parts)
                ref[side, unit, AT_DOC : AT_DOC + 16, :] = jnp.concatenate([head, parts], axis=0).astype(BF16)

    def prepare_keys(plane):
        row, col = iota((TILE, D), 0), iota((TILE, D), 1)
        for t in range(TILES):
            position = order[plane * TILES + t] * BLOCK + quarter * TILE + row
            hot = col == plane * TILES + t
            hot = hot | (doc_lane & (position >= spans[0:1, :]) & (position < spans[1:2, :]))
            hot = hot | ((col >= AT_ONE) & (col < AT_ONE + 3))
            ax[plane, pl.ds(t * TILE, TILE), :] = hot.astype(F32).astype(BF16)

    def spot(n):
        side = n // 32
        j = n % 32 // 4
        j = j + side * (7 - 2 * j)
        unit = n % 4
        m = n - 52
        late = jnp.where(m >= 0, 1, 0)
        k = m // 3
        j = j + late * (2 - m % 3 - j)
        unit = unit + late * ((k // 2 * (2 * c - 1) + 1 - c) * 2 + k % 2 - unit)
        away = (j + 1) // 2
        return (z + NZ + away * (1 - 2 * (j % 2))) % NZ, side, unit

    def front(n):
        plane, side, unit = spot(n)
        extra = ax[plane]
        scores = dot(
            jnp.concatenate([kv[0, plane], extra], 1), jnp.concatenate([qt[side, unit], qx[side, unit]], 0), NN
        )
        grads_less = dot(
            jnp.concatenate([kv[1, plane], extra], 1), jnp.concatenate([gt[side, unit], gx[side, unit]], 0), NN
        )
        low, score_grad = [], []
        for t in range(TILES):
            part = slice(t * TILE, (t + 1) * TILE)
            bound = []
            for b in range(2):
                same = order[plane * TILES + t] == order[z * 8 + unit * 2 + b]
                bound.append(jnp.full((1, 2 * BLOCK), jnp.where(same, 0, ALWAYS), jnp.int32))
            visible = ahead[...] <= jnp.concatenate(bound, axis=1)
            weights = jnp.where(visible, jnp.exp2(scores[part, :] * (SCALE * LOG2E)), 0.0)
            low.append(weights.astype(BF16))
            score_grad.append((weights * grads_less[part, :]).astype(BF16))
        return jnp.concatenate(low, axis=0), jnp.concatenate(score_grad, axis=0)

    def back(n, low, score_grad):
        plane, side, unit = spot(n)
        acc[0, plane] += dot(qt[side, unit], score_grad, NT)
        acc[1, plane] += dot(gt[side, unit], low, NT)
        dqt[side, unit] += dot(kv[0, plane], score_grad, TN)

    def query_sums(side, cb, blocks=range(4)):
        for rb in blocks:
            for hh in range(2):
                at = (rb % 2 * 2 + hh) * BLOCK
                block_grad = dqt[side, cb * 2 + rb // 2, :, at : at + BLOCK].T * SCALE
                dqp[side, cb, rb * BLOCK : (rb + 1) * BLOCK, hh * D : (hh + 1) * D] = block_grad

    def key_copy(way, step, t):
        piece = kv.at[t, under[step - 1] if way == 0 else above[step - 1]]
        return send(
            piece, piece, k_send.at[way, step - 1, t], k_recv.at[way, step - 1, t],
            up if way == 0 else down, h,
        )

    def carries(way, step, t):
        return step < 4 or (step == 4 and t == way)

    def arrive(step, t):
        for way in range(2):
            if carries(way, step, t):
                key_copy(way, step, t).wait_recv()
            if carries(way, step + 1, t):
                key_copy(way, step + 1, t).start()

    def forward(k):
        src = (qt.at[1, mine], gt.at[1, mine], None, st.at[1, c])[k]
        return send(src, src, f_send.at[k], f_recv.at[k], twin, h)

    def pass_on(k):
        y_copy(k).wait_recv()
        forward(k).start()

    def sum_copy(way, step, t):
        return send(
            z_out.at[way, step - 1, t], z_in.at[way, step - 1, t],
            z_send.at[way, step - 1, t], z_recv.at[way, step - 1, t],
            up if way == 0 else down, h,
        )

    def pass_sum(way, step, t):
        value = acc[t, (above if way == 0 else under)[5 - step]]
        if step > 2 or (step == 2 and t == way):
            sum_copy(way, step - 1, t).wait_recv()
            value = value + z_in[way, step - 2, t].astype(F32)
        z_out[way, step - 1, t] = value.astype(BF16)
        sum_copy(way, step, t).start()

    def twin_copy(side):
        return send(dqp.at[side, 1 - c], twin_in.at[side], r_send.at[side], r_recv.at[side], twin, h)

    def twin_sums(side):
        query_sums(side, 1 - c)
        twin_copy(side).start()

    def pair_copy(rp):
        rows = pl.ds(rp * 2 * BLOCK, 2 * BLOCK)
        return send(
            pair_out.at[rows, :], pair_in.at[rows, :], r_send.at[2 + rp], r_recv.at[2 + rp], s, pair
        )

    def pair_sums(rp):
        query_sums(1, c, range(rp * 2, rp * 2 + 2))
        if rp == 0:
            twin_copy(1).wait_recv()
        rows = slice(rp * 2 * BLOCK, (rp + 1) * 2 * BLOCK)
        pair_out[rows, :] = (dqp[1, c, rows, :] + twin_in[1, rows, :]).astype(BF16)
        pair_copy(rp).start()

    mine_g = x * 2 + y // 2

    def way_copy(way, t, k, seq, head):
        return send(
            fin.at[way, k, t], way_in.at[way, mine_g, t],
            w_send.at[way, t, k], w_recv.at[way, t, mine_g], seq, head,
        )

    def last_sum(way, t):
        plane = (above if way == 0 else under)[1]
        sum_copy(way, 3, t).wait_recv()
        value = (acc[t, plane] + z_in[way, 2, t].astype(F32)).T.astype(BF16)
        for k, (seq, head, _) in enumerate(givers(plane)):
            fin[way, k, t] = value[k * TILE : (k + 1) * TILE, :]
        for k, (seq, head, _) in enumerate(givers(plane)):
            way_copy(way, t, k, seq, head).start()

    prepare(0, c)
    for plane in near:
        prepare_keys(plane)
    for copy in d_copies:
        copy.wait_recv()
    prepare(0, 1 - c)
    for t in range(2):
        rows_come(0, t)
        for way in range(2):
            rows_come(1 + way, t)
            key_copy(way, 2, t).start()
    lows[0], sgs[0] = front(z * 0)

    def planes_at(away):
        prepare_keys(under[away])
        if away < 4:
            prepare_keys(above[away])

    def heads_come():
        pass_on(1)
        pass_on(3)
        y_copy(2).wait_recv()

    def other_heads():
        lperm[1] = dot(l_in[...], stored, NN)
        prepare(1, c)
        for k in (0, 1, 3):
            forward(k).wait_recv()
        prepare(1, 1 - c)

    def sums(*which):
        for w in which:
            pass_sum(*w)

    events = {
        4: lambda: (planes_at(2), arrive(2, 0)),
        5: lambda: arrive(2, 1),
        6: lambda: pass_on(0),
        8: lambda: (planes_at(3), arrive(3, 0)),
        9: lambda: arrive(3, 1),
        11: lambda: (planes_at(4), arrive(4, 0)),
        13: lambda: (heads_come(), arrive(4, 1)),
        15: lambda: other_heads(),
        18: lambda: sums((0, 1, 0), (1, 1, 1)),
        20: lambda: sums((0, 2, 1)),
        21: lambda: twin_sums(0),
        22: lambda: sums((0, 2, 0), (1, 2, 0), (1, 2, 1)),
        24: lambda: sums((0, 3, 1)),
        26: lambda: sums((0, 3, 0), (1, 3, 0)),
        28: lambda: sums((1, 3, 1)),
        29: lambda: twin_sums(1),
        31: lambda: (last_sum(0, 1), last_sum(0, 0), pair_sums(0)),
    }

    def pair_of_steps(i):
        n = 2 * i
        lows[1], sgs[1] = front(n + 1)
        back(n, lows[0], sgs[0])
        lows[0], sgs[0] = front(jnp.minimum(n + 2, 63))
        back(n + 1, lows[1], sgs[1])

    def happen(i, steps):
        if len(steps) == 1:
            pl.when(i == steps[0])(lambda: (events[steps[0]](), None)[1])
        else:
            mid = len(steps) // 2
            lax.cond(i < steps[mid], lambda: happen(i, steps[:mid]), lambda: happen(i, steps[mid:]))

    def steps_between(lo, hi):
        def two(i, _):
            happen(i, [at for at in sorted(events) if lo <= at < hi])
            pair_of_steps(i)
            return 0

        lax.fori_loop(lo, hi, two, 0)

    steps_between(0, 16)
    steps_between(16, 32)

    last_sum(1, 0)
    last_sum(1, 1)
    pair_sums(1)

    for t in range(2):
        value = acc[t, z].T.astype(BF16)
        for k in range(8):
            fin[2, k, t] = value[k * TILE : (k + 1) * TILE, :]
        for k, (seq, head, other) in enumerate(givers(z)):
            pl.when(other)(way_copy(2, t, k, seq, head).start)

            @pl.when(jnp.logical_not(other))
            def _():
                way_in[2, mine_g, t] = fin[2, k, t]

    query_sums(0, c)
    twin_copy(0).wait_recv()
    dq[...] = dqp[0, c] + twin_in[0]

    for way, plane in enumerate((under[1], above[1], z)):
        for t in range(2):
            for g, (seq, head, other) in enumerate(takers(plane)):
                landed = send(
                    fin.at[way, 0, t], way_in.at[way, g, t],
                    w_send.at[way, t, 0], w_recv.at[way, t, g], seq, head,
                )
                pl.when(other)(landed.wait_recv)
    for rp in range(2):
        pair_copy(rp).wait_recv()

    for o, plane in enumerate(near):
        for g, (seq, head, other) in enumerate(takers(plane)):
            for t in range(2):
                pl.when(other)(row_copy(o, t, g, seq, head).wait_send)
    for way, plane in enumerate((above[1], under[1], z)):
        for t in range(2):
            for k, (seq, head, other) in enumerate(givers(plane)):
                pl.when(other)(way_copy(way, t, k, seq, head).wait_send)
    for way in range(2):
        for t in range(2):
            for step in range(2, 5):
                if carries(way, step, t):
                    key_copy(way, step, t).wait_send()
            for step in range(1, 4):
                if step > 1 or t == way:
                    sum_copy(way, step, t).wait_send()
    for k in range(4):
        y_copy(k).wait_send()
        if k != 2:
            forward(k).wait_send()
    for copy in d_copies + [twin_copy(0), twin_copy(1), pair_copy(0), pair_copy(1)]:
        copy.wait_send()


def fused(keys, values, queries, grads, outs, norms, layout, ids, order):
    vmem = pl.BlockSpec(memory_space=pltpu.VMEM)
    hbm = pl.BlockSpec(memory_space=pltpu.HBM)
    dma = pltpu.SemaphoreType.DMA
    v = pltpu.VMEM
    return pl.pallas_call(
        fused_kernel,
        name="fused",
        out_shape=(
            jax.ShapeDtypeStruct((ROWS, 2 * D), F32),
            jax.ShapeDtypeStruct((ROWS, 2 * D), BF16),
            jax.ShapeDtypeStruct((3, 8, 2, TILE, D), BF16),
        ),
        in_specs=[hbm] * 9,
        out_specs=(vmem,) * 3,
        scratch_shapes=[
            v((TILE, 8 * D), BF16), v((TILE, 8 * D), BF16),
            v((ROWS, 2 * D), BF16), v((ROWS, 2 * D), BF16), v((ROWS, 2 * D), BF16),
            v((2, ROWS), F32), v((2, NBLK, NBLK), jnp.int32),
            v((NBLK, BLOCK), jnp.int32), pltpu.SMEM((NBLK,), jnp.int32), v((1, D), jnp.int32),
            v((2, NZ, PLANE, D), BF16),
            v((2, 4, D, COLS), BF16), v((2, 4, D, COLS), BF16),
            v((2, 2, 16, BLOCK), F32),
            v((2 * NBLK, NBLK), BF16), v((2 * NBLK, NBLK), BF16),
            v((2, 2 * NBLK, D), F32), v((8, D), jnp.int32), v((2, 8, COLS), jnp.int32),
            v((NZ, PLANE, D), BF16),
            v((2, 4, D, COLS), BF16), v((2, 4, D, COLS), BF16),
            v((2, PLANE, COLS), BF16), v((2, PLANE, COLS), BF16),
            v((2, NZ, D, PLANE), F32),
            v((2, 4, D, COLS), F32),
            v((2, 2, ROWS, 2 * D), F32),
            v((2, ROWS, 2 * D), F32), v((ROWS, 2 * D), BF16),
            v((2, 4, 2, D, PLANE), BF16), v((2, 4, 2, D, PLANE), BF16),
            v((3, 8, 2, TILE, D), BF16),
            v((TILE, COLS), jnp.int32), v((8, D), F32),
            dma((9,)), dma((3, 2, 8)), dma((3, 2, 8)),
            dma((2, 4, 2)), dma((2, 4, 2)), dma((2, 4, 2)), dma((2, 4, 2)),
            dma((4,)), dma((4,)), dma((3,)), dma((3,)),
            dma((4,)), dma((4,)), dma((4,)), dma((4,)), dma((3, 2, 8)), dma((3, 2, 8)),
        ],
        compiler_params=pltpu.CompilerParams(
            collective_id=0, has_side_effects=True, vmem_limit_bytes=60 * MIB
        ),
    )(keys, values, queries, grads, outs, norms, layout, ids, order)


def finish_kernel(sums, pair_in, way_in, dq, dk, dv):
    dq[...] = sums[...] + pair_in[...].astype(F32)
    for g in range(8):
        for t, (ref, scale) in enumerate(((dk, SCALE), (dv, 1.0))):
            total = way_in[2, g, t].astype(F32) + way_in[0, g, t].astype(F32) + way_in[1, g, t].astype(F32)
            ref[:, g * D : (g + 1) * D] = total * scale


def finish(sums, pair_in, way_in):
    vmem = pl.BlockSpec(memory_space=pltpu.VMEM)
    return pl.pallas_call(
        finish_kernel,
        name="finish",
        out_shape=(
            jax.ShapeDtypeStruct((ROWS, 2 * D), F32),
            jax.ShapeDtypeStruct((TILE, 8 * D), F32),
            jax.ShapeDtypeStruct((TILE, 8 * D), F32),
        ),
        in_specs=[vmem] * 3,
        out_specs=(vmem,) * 3,
        compiler_params=pltpu.CompilerParams(vmem_limit_bytes=60 * MIB),
    )(sums, pair_in, way_in)


def body(
    queries, keys, values, attn_out, out_grad, log_norm, block_layout, document_ids, block_order
):
    return finish(
        *fused(
            keys,
            values,
            queries,
            out_grad,
            attn_out,
            log_norm,
            block_layout,
            document_ids.reshape(NBLK, BLOCK),
            block_order,
        )
    )


def solution(mesh):
    in_specs = (
        P("seq", "head"),
        P(("seq", "head"), None),
        P(("seq", "head"), None),
        P("seq", "head"),
        P("seq", "head"),
        P("head", "seq"),
        P("head", None, None),
        P(),
        P(),
    )
    out_specs = (P("seq", "head"), P(("seq", "head"), None), P(("seq", "head"), None))
    return jax.shard_map(body, mesh=mesh, in_specs=in_specs, out_specs=out_specs, check_vma=False)
```
